32 devices in a mesh: node: 16 (over z, x, core), col: 2 (over y).
Axes of the slice: x: 2, y: 2, z: 4, core: 2. Of those that a mesh axis runs over, the one named last changes fastest.
Arguments:
- coefficients: float32 [2, 64, 256, 1024], P('col', 'node'), may hold values from -6 to 6
- self_weights: bfloat16 [2, 6, 64, 256, 256], P('col', None, 'node'), may hold values from -0.25 to 0.25
- cross_weights: bfloat16 [2, 6, 64, 256, 256], P('col', None, 'node'), may hold values from -0.25 to 0.25
- true_ranks: int32 [2, 64], P('col', 'node'), may hold values from 128 to 256
Outputs:
- field: float32 [64, 256, 1024], P('node', None, 'col')
The draws below stay inside these ranges and needn't reach their ends.
Inputs may be any that keep to these rules, and one draw needn't show every extreme that they name: `true_ranks`: each node's true rank within its padded rank 256.
All inputs are finite; a program needn't handle non-finite values.
Results may differ from the reference program's by a relative error of at most 0.0003.
Values sent between devices are 32-bit elements; how exact they have to be, the bound alone decides.
A program may use at most 64 MiB of HBM per device.

```python
import jax
import jax.numpy as jnp
from jax import lax

RANK = 256
ILLUM = 1024
LEVELS = 6
NODES = 64
COLS = 2


def place_ends(result, own_key, smallest, top_value):
    longest = result.shape.index(max(result.shape))
    spots = []
    for shift in (0, 1):
        where = [jax.random.randint(jax.random.fold_in(own_key, axis), (), 0, length) for axis, length in enumerate(result.shape)]
        where[longest] = (where[longest] + shift) % result.shape[longest]
        spots.append(tuple(where))
    return result.at[spots[0]].set(smallest).at[spots[1]].set(top_value)


def block_scale(key, extent, shards, smallest, high):
    def one(position, parts):
        steps = jax.random.uniform(jax.random.fold_in(jax.random.fold_in(key, 6), position), (parts,), jnp.float32, smallest / len(shards), high / len(shards))
        return jnp.repeat(jnp.exp(steps), extent[position] // parts).reshape((-1,) + (1,) * (len(extent) - position - 1))

    loudness = one(*shards[0])
    for cut in shards[1:]:
        loudness = loudness * one(*cut)
    return loudness


def gaussian(own_key, dims, deviation, reach, split=(), held_as=jnp.bfloat16):
    drawn = jax.random.normal(own_key, dims, jnp.float32) * deviation
    if len(split) > 0:
        drawn = block_scale(own_key, dims, split, -0.22, 0.18) * drawn
    return jnp.clip(drawn, min=-reach, max=reach).astype(held_as)


def setup_inputs(seed: int = 0) -> dict:
    key_list = jax.random.split(jax.random.key(seed), 5)
    return {
        "coefficients": gaussian(key_list[0], (COLS, NODES, RANK, ILLUM), 1.0, 6.0, ((0, 2), (1, 16)), jnp.float32),
        "self_weights": gaussian(key_list[1], (COLS, LEVELS, NODES, RANK, RANK), (2 * RANK) ** -0.5, 0.25, ((0, 2), (2, 16))),
        "cross_weights": gaussian(key_list[2], (COLS, LEVELS, NODES, RANK, RANK), (2 * RANK) ** -0.5, 0.25, ((0, 2), (2, 16))),
        "true_ranks": place_ends(jax.random.randint(key_list[3], (COLS, NODES), RANK // 2, RANK + 1), jax.random.fold_in(key_list[3], 1), RANK // 2, RANK).astype(jnp.int32),
    }


def apply_mats(weights, coeffs):
    return jnp.einsum("nrk,nki->nri", weights.astype(jnp.float32), coeffs, precision=lax.Precision.HIGHEST)


def partner_view(values, section):
    node_count = values.shape[0]
    shaped = values.reshape((node_count >> (section + 1), 2, 1 << section) + values.shape[1:])
    return shaped[:, ::-1].reshape(values.shape)


def reference(coefficients, self_weights, cross_weights, true_ranks):
    def column(running, items):
        coeffs, self_mats, cross_mats, rank_vec = items
        row_index = lax.broadcasted_iota(jnp.int32, (coeffs.shape[0], coeffs.shape[1], 1), 1)
        row_keep = (row_index < rank_vec.astype(jnp.int32)[:, None, None]).astype(jnp.float32)
        for section in range(LEVELS):
            self_term = apply_mats(self_mats[section], coeffs)
            sent_term = apply_mats(cross_mats[section], coeffs)
            coeffs = row_keep * (self_term + partner_view(sent_term, section))
        return running + coeffs, None

    start = jnp.zeros(coefficients.shape[1:], jnp.float32)
    running, _ = lax.scan(column, start, (coefficients, self_weights, cross_weights, true_ranks))
    return running
```

```python
import functools

import jax
import jax.numpy as jnp
from jax import lax
from jax.experimental import pallas as pl
from jax.experimental.pallas import tpu as pltpu
from jax.sharding import PartitionSpec as P

WIDTH = 128
LAG = 4


def flip(index, mask):
    return index + mask * (1 - 2 * ((index // mask) % 2))


def split(state):
    high = state.astype(jnp.bfloat16)
    low = (state - high.astype(jnp.float32)).astype(jnp.bfloat16)
    return high, low


def product(weights, parts):
    high, low = parts
    return jnp.dot(weights, high, preferred_element_type=jnp.float32) + jnp.dot(
        weights, low, preferred_element_type=jnp.float32
    )


def kernel(
    cols, nodes, levels, width, shard,
    coeff, self_hbm, cross_hbm, ranks, out,
    acc, tmp, self_w, cross_w, send, recv, col_send, col_recv, end_send, end_recv,
    own_rank, other_rank,
    load_sem, weight_sem, send_sem, recv_sem, col_send_sem, col_recv_sem,
    end_send_sem, end_recv_sem, rank_sem,
):
    rank_rows = acc.shape[1]
    local_bits = nodes.bit_length() - 1
    hops = levels - local_bits
    pieces = shard // width
    chunks = cols * pieces
    items = chunks * nodes
    theirs = (cols - 1) * pieces * nodes
    me = lax.axis_index("node")
    my_col = lax.axis_index("col")
    peers = [flip(me, 1 << hop) for hop in range(hops)]

    def load(chunk):
        column = (my_col + 1 + chunk % cols) % cols
        start = pl.multiple_of(column * shard + (chunk // cols) * width, width)
        return pltpu.make_async_copy(
            coeff.at[0, :, :, pl.ds(start, width)],
            acc.at[pl.ds(chunk * nodes, nodes)],
            load_sem.at[chunk],
        )

    def weight_loads(level):
        return (
            pltpu.make_async_copy(self_hbm.at[0, level], self_w.at[level], weight_sem.at[0, level]),
            pltpu.make_async_copy(cross_hbm.at[0, level], cross_w.at[level], weight_sem.at[1, level]),
        )

    def hop_copy(hop, item):
        return pltpu.make_async_remote_copy(
            src_ref=send.at[hop, item],
            dst_ref=recv.at[hop, item],
            send_sem=send_sem.at[hop, item],
            recv_sem=recv_sem.at[hop, item],
            device_id={"node": peers[hop]},
            device_id_type=pl.DeviceIdType.MESH,
        )

    def col_copy(item):
        column = (my_col + 1 + (item // nodes) % (cols - 1)) % cols
        return pltpu.make_async_remote_copy(
            src_ref=col_send.at[item],
            dst_ref=col_recv.at[item],
            send_sem=col_send_sem.at[item],
            recv_sem=col_recv_sem.at[item],
            device_id={"col": column},
            device_id_type=pl.DeviceIdType.MESH,
        )

    def end_copy(place):
        return pltpu.make_async_remote_copy(
            src_ref=end_send.at[place],
            dst_ref=end_recv.at[place],
            send_sem=end_send_sem.at[place],
            recv_sem=end_recv_sem.at[place],
            device_id={"node": peers[hops - 1]},
            device_id_type=pl.DeviceIdType.MESH,
        )

    rank_copy = pltpu.make_async_remote_copy(
        src_ref=own_rank,
        dst_ref=other_rank,
        send_sem=rank_sem.at[0],
        recv_sem=rank_sem.at[1],
        device_id={"node": peers[hops - 1]},
        device_id_type=pl.DeviceIdType.MESH,
    )

    load(0).start()
    for level in range(local_bits + 1):
        for copy in weight_loads(level):
            copy.start()
    for chunk in range(1, chunks):
        load(chunk).start()
    for level in range(local_bits + 1, levels):
        for copy in weight_loads(level):
            copy.start()

    barrier = pltpu.get_barrier_semaphore()
    for peer in peers:
        pl.semaphore_signal(barrier, inc=1, device_id={"node": peer}, device_id_type=pl.DeviceIdType.MESH)
    for step in range(1, cols):
        pl.semaphore_signal(
            barrier, inc=1, device_id={"col": (my_col + step) % cols}, device_id_type=pl.DeviceIdType.MESH
        )
    for node in range(nodes):
        own_rank[node] = jnp.full(own_rank.shape[1:], ranks[0, node], jnp.int32)
    pl.semaphore_wait(barrier, hops + cols - 1)
    rank_copy.start()

    row = lax.broadcasted_iota(jnp.int32, (rank_rows, width), 0)

    def masked(values, rank_tile):
        return jnp.where(row < rank_tile[0:1, :], values, 0.0)

    def first(chunk):
        base = chunk * nodes
        load(chunk).wait()

        def at(bank, node):
            return acc.at[base + node] if bank == 0 else tmp.at[node]

        for level in range(local_bits):

            @pl.when(chunk == 0)
            def _():
                for copy in weight_loads(level):
                    copy.wait()

            def body(node, _):
                other = flip(node, 1 << level)
                value = product(self_w[level, node], split(at(level % 2, node)[...]))
                value += product(cross_w[level, other], split(at(level % 2, other)[...]))
                at((level + 1) % 2, node)[...] = masked(value, own_rank[node])
                return 0

            lax.fori_loop(0, nodes, body, 0)

        @pl.when(chunk == 0)
        def _():
            for copy in weight_loads(local_bits):
                copy.wait()

        def body(node, _):
            parts = split(at(local_bits % 2, node)[...])
            send[0, base + node] = product(cross_w[local_bits, node], parts)
            hop_copy(0, base + node).start()
            acc[base + node] = product(self_w[local_bits, node], parts)
            return 0

        lax.fori_loop(0, nodes, body, 0)

    def combine(hop, item):
        level = local_bits + hop

        @pl.when(item == 0)
        def _():
            for copy in weight_loads(level):
                copy.wait()

        hop_copy(hop - 1, item).wait_recv()
        node = item % nodes
        return node, level, split(masked(acc[item] + recv[hop - 1, item], own_rank[node]))

    def middle(hop, item):
        node, level, parts = combine(hop, item)
        send[hop, item] = product(cross_w[level, node], parts)
        hop_copy(hop, item).start()
        acc[item] = product(self_w[level, node], parts)

    def last(item):
        node, level, parts = combine(hops - 1, item)

        @pl.when(item == 0)
        def _():
            rank_copy.wait()

        sent = masked(product(cross_w[level, node], parts), other_rank[node])
        kept = masked(product(self_w[level, node], parts), own_rank[node])

        chunk = item // nodes
        piece = chunk // cols

        @pl.when(chunk % cols < cols - 1)
        def _():
            slot = (piece * (cols - 1) + chunk % cols) * nodes + node
            col_send[slot, 0] = kept
            col_send[slot, 1] = sent
            col_copy(slot).start()

        @pl.when(chunk % cols == cols - 1)
        def _():
            place = piece * nodes + node
            total_kept, total_sent = kept, sent
            for step in range(cols - 1):
                slot = (piece * (cols - 1) + step) * nodes + node
                col_copy(slot).wait_recv()
                total_kept += col_recv[slot, 0]
                total_sent += col_recv[slot, 1]
            end_send[place] = total_sent
            end_copy(place).start()
            acc[item] = total_kept

    def finish(item):
        node = item % nodes
        piece = item // (nodes * cols)
        place = piece * nodes + node
        end_copy(place).wait_recv()
        start = pl.multiple_of(piece * width, width)
        out[node, :, pl.ds(start, width)] = acc[item] + end_recv[place]

    def tick(time, _):
        @pl.when((time < items) & (time % nodes == 0))
        def _():
            first(time // nodes)

        for hop in range(1, hops):
            item = time - (1 + (hop - 1) * LAG)

            @pl.when((item >= 0) & (item < items))
            def _():
                if hop == hops - 1:
                    last(item)
                else:
                    middle(hop, item)

        done = time - (1 + (hops - 1) * LAG)

        @pl.when((done >= 0) & ((done // nodes) % cols == cols - 1))
        def _():
            finish(done)

        return 0

    lax.fori_loop(0, items + 1 + (hops - 1) * LAG, tick, 0)

    def drain_hops(item, _):
        for hop in range(hops - 1):
            hop_copy(hop, item).wait_send()
        return 0

    def drain_cols(item, _):
        col_copy(item).wait_send()
        return 0

    def drain_end(place, _):
        end_copy(place).wait_send()
        return 0

    lax.fori_loop(0, items, drain_hops, 0)
    lax.fori_loop(0, theirs, drain_cols, 0)
    lax.fori_loop(0, items - theirs, drain_end, 0)


def shards(cols, coefficients, self_weights, cross_weights, true_ranks):
    nodes, rank, illum = coefficients.shape[1:]
    levels = self_weights.shape[1]
    shard = illum // cols
    width = min(WIDTH, shard)
    items = illum // width * nodes
    mine = shard // width * nodes
    theirs = items - mine
    hops = levels - (nodes.bit_length() - 1)
    tile = (rank, width)
    dma = pltpu.SemaphoreType.DMA
    return pl.pallas_call(
        functools.partial(kernel, cols, nodes, levels, width, shard),
        out_shape=jax.ShapeDtypeStruct((nodes, rank, shard), jnp.float32),
        in_specs=[pl.BlockSpec(memory_space=pl.ANY)] * 3 + [pl.BlockSpec(memory_space=pltpu.SMEM)],
        out_specs=pl.BlockSpec(memory_space=pltpu.VMEM),
        scratch_shapes=[
            pltpu.VMEM((items, *tile), jnp.float32),
            pltpu.VMEM((nodes, *tile), jnp.float32),
            pltpu.VMEM((levels, nodes, rank, rank), jnp.bfloat16),
            pltpu.VMEM((levels, nodes, rank, rank), jnp.bfloat16),
            pltpu.VMEM((hops - 1, items, *tile), jnp.float32),
            pltpu.VMEM((hops - 1, items, *tile), jnp.float32),
            pltpu.VMEM((theirs, 2, *tile), jnp.float32),
            pltpu.VMEM((theirs, 2, *tile), jnp.float32),
            pltpu.VMEM((mine, *tile), jnp.float32),
            pltpu.VMEM((mine, *tile), jnp.float32),
            pltpu.VMEM((nodes, 8, width), jnp.int32),
            pltpu.VMEM((nodes, 8, width), jnp.int32),
            dma((items // nodes,)),
            dma((2, levels)),
            dma((hops - 1, items)),
            dma((hops - 1, items)),
            dma((theirs,)),
            dma((theirs,)),
            dma((mine,)),
            dma((mine,)),
            dma((2,)),
        ],
        compiler_params=pltpu.CompilerParams(
            collective_id=0, has_side_effects=True, vmem_limit_bytes=51 * 1024 * 1024
        ),
    )(coefficients, self_weights, cross_weights, true_ranks)


def solution(mesh):
    placed = (
        P("col", "node", None, None),
        P("col", None, "node", None, None),
        P("col", None, "node", None, None),
        P("col", "node"),
    )
    return jax.shard_map(
        functools.partial(shards, mesh.shape["col"]),
        mesh=mesh, in_specs=placed, out_specs=P("node", None, "col"), check_vma=False,
    )
```

```python
import functools

import jax
import jax.numpy as jnp
from jax import lax
from jax.experimental import pallas as pl
from jax.experimental.pallas import tpu as pltpu
from jax.sharding import PartitionSpec as P

WIDTH = 128
GROUP = 2
LAGS = (1, 4, 4)


def flip(index, mask):
    return index + mask * (1 - 2 * ((index // mask) % 2))


def split(state):
    high = state.astype(jnp.bfloat16)
    low = (state - high.astype(jnp.float32)).astype(jnp.bfloat16)
    return high, low


def product(weights, parts):
    high, low = parts
    return jnp.dot(weights, high, preferred_element_type=jnp.float32) + jnp.dot(
        weights, low, preferred_element_type=jnp.float32
    )


def kernel(
    cols, nodes, levels, width, shard,
    coeff, self_hbm, cross_hbm, ranks, out,
    acc, tmp, self_w, cross_w, send, recv, col_send, col_recv, end_send, end_recv,
    own_rank, other_rank,
    load_sem, weight_sem, send_sem, recv_sem, col_send_sem, col_recv_sem,
    end_send_sem, end_recv_sem, rank_sem,
):
    rank_rows = acc.shape[1]
    local_bits = nodes.bit_length() - 1
    hops = levels - local_bits
    pieces = shard // width
    chunks = cols * pieces
    items = chunks * nodes
    theirs = (cols - 1) * pieces * nodes
    me = lax.axis_index("node")
    my_col = lax.axis_index("col")
    peers = [flip(me, 1 << hop) for hop in range(hops)]

    def load(chunk):
        column = (my_col + 1 + chunk % cols) % cols
        start = pl.multiple_of(column * shard + (chunk // cols) * width, width)
        return pltpu.make_async_copy(
            coeff.at[0, :, :, pl.ds(start, width)],
            acc.at[pl.ds(chunk * nodes, nodes)],
            load_sem.at[chunk],
        )

    def weight_loads(level):
        return (
            pltpu.make_async_copy(self_hbm.at[0, level], self_w.at[level], weight_sem.at[0, level]),
            pltpu.make_async_copy(cross_hbm.at[0, level], cross_w.at[level], weight_sem.at[1, level]),
        )

    def hop_copy(hop, item):
        return pltpu.make_async_remote_copy(
            src_ref=send.at[hop, item],
            dst_ref=recv.at[hop, item],
            send_sem=send_sem.at[hop, item],
            recv_sem=recv_sem.at[hop, item],
            device_id={"node": peers[hop]},
            device_id_type=pl.DeviceIdType.MESH,
        )

    def col_copy(item):
        column = (my_col + 1 + (item // nodes) % (cols - 1)) % cols
        return pltpu.make_async_remote_copy(
            src_ref=col_send.at[item],
            dst_ref=col_recv.at[item],
            send_sem=col_send_sem.at[item],
            recv_sem=col_recv_sem.at[item],
            device_id={"col": column},
            device_id_type=pl.DeviceIdType.MESH,
        )

    def end_copy(place):
        return pltpu.make_async_remote_copy(
            src_ref=end_send.at[place],
            dst_ref=end_recv.at[place],
            send_sem=end_send_sem.at[place],
            recv_sem=end_recv_sem.at[place],
            device_id={"node": peers[hops - 1]},
            device_id_type=pl.DeviceIdType.MESH,
        )

    rank_copy = pltpu.make_async_remote_copy(
        src_ref=own_rank,
        dst_ref=other_rank,
        send_sem=rank_sem.at[0],
        recv_sem=rank_sem.at[1],
        device_id={"node": peers[hops - 1]},
        device_id_type=pl.DeviceIdType.MESH,
    )

    for chunk in range(GROUP):
        load(chunk).start()
    for level in range(local_bits + 1):
        for copy in weight_loads(level):
            copy.start()
    for chunk in range(GROUP, chunks):
        load(chunk).start()
    for level in range(local_bits + 1, levels):
        for copy in weight_loads(level):
            copy.start()

    barrier = pltpu.get_barrier_semaphore()
    for peer in peers:
        pl.semaphore_signal(barrier, inc=1, device_id={"node": peer}, device_id_type=pl.DeviceIdType.MESH)
    for step in range(1, cols):
        pl.semaphore_signal(
            barrier, inc=1, device_id={"col": (my_col + step) % cols}, device_id_type=pl.DeviceIdType.MESH
        )
    for node in range(nodes):
        own_rank[node] = jnp.full(own_rank.shape[1:], ranks[0, node], jnp.int32)
    pl.semaphore_wait(barrier, hops + cols - 1)
    rank_copy.start()

    row = lax.broadcasted_iota(jnp.int32, (rank_rows, width), 0)

    def masked(values, rank_tile):
        return jnp.where(row < rank_tile[0:1, :], values, 0.0)

    def state(bank, chunk, node):
        return acc.at[chunk * nodes + node] if bank == 0 else tmp.at[chunk % GROUP, node]

    def stack(bank, pair, node):
        halves = [split(state(bank, pair * GROUP + part, node)[...]) for part in range(GROUP)]
        return tuple(jnp.concatenate(half, axis=1) for half in zip(*halves))

    def columns(values, part):
        return values[:, part * width : (part + 1) * width]

    def local(pair):
        for part in range(GROUP):
            load(pair * GROUP + part).wait()
        for level in range(local_bits):

            @pl.when(pair == 0)
            def _():
                for copy in weight_loads(level):
                    copy.wait()

            for node in range(nodes):
                other = node + (1 << level)
                if (node >> level) % 2:
                    continue
                mine, theirs = stack(level % 2, pair, node), stack(level % 2, pair, other)
                for to, at, source in ((node, mine, theirs), (other, theirs, mine)):
                    value = product(self_w[level, to], at)
                    value += product(cross_w[level, node + other - to], source)
                    for part in range(GROUP):
                        state((level + 1) % 2, pair * GROUP + part, to)[...] = masked(
                            columns(value, part), own_rank[to]
                        )

        @pl.when(pair == 0)
        def _():
            for copy in weight_loads(local_bits):
                copy.wait()

    def first(step):
        pair, node = step // nodes, step % nodes
        parts = stack(local_bits % 2, pair, node)
        value = product(cross_w[local_bits, node], parts)
        for part in range(GROUP):
            send[0, (pair * GROUP + part) * nodes + node] = columns(value, part)
            hop_copy(0, (pair * GROUP + part) * nodes + node).start()
        value = product(self_w[local_bits, node], parts)
        for part in range(GROUP):
            acc[(pair * GROUP + part) * nodes + node] = columns(value, part)

    def combine(hop, item, lead):
        level = local_bits + hop

        @pl.when(lead)
        def _():
            for copy in weight_loads(level):
                copy.wait()

        hop_copy(hop - 1, item).wait_recv()
        node = item % nodes
        high, low = split(masked(acc[item] + recv[hop - 1, item], own_rank[node]))
        return node, level, jnp.concatenate([high, low], axis=1)

    def wide(weights, parts):
        both = jnp.dot(weights, parts, preferred_element_type=jnp.float32)
        return both[:, :width] + both[:, width:]

    def middle(hop, item, lead):
        node, level, parts = combine(hop, item, lead)
        send[hop, item] = wide(cross_w[level, node], parts)
        hop_copy(hop, item).start()
        acc[item] = wide(self_w[level, node], parts)

    def last(item, lead):
        node, level, parts = combine(hops - 1, item, lead)

        @pl.when(lead)
        def _():
            rank_copy.wait()

        sent = masked(wide(cross_w[level, node], parts), other_rank[node])
        kept = masked(wide(self_w[level, node], parts), own_rank[node])

        chunk = item // nodes
        piece = chunk // cols

        @pl.when(chunk % cols < cols - 1)
        def _():
            slot = (piece * (cols - 1) + chunk % cols) * nodes + node
            col_send[slot, 0] = kept
            col_send[slot, 1] = sent
            col_copy(slot).start()

        @pl.when(chunk % cols == cols - 1)
        def _():
            place = piece * nodes + node
            total_kept, total_sent = kept, sent
            for step in range(cols - 1):
                slot = (piece * (cols - 1) + step) * nodes + node
                col_copy(slot).wait_recv()
                total_kept += col_recv[slot, 0]
                total_sent += col_recv[slot, 1]
            end_send[place] = total_sent
            end_copy(place).start()
            acc[item] = total_kept

    def finish(item):
        node = item % nodes
        piece = item // (nodes * cols)
        place = piece * nodes + node
        end_copy(place).wait_recv()
        start = pl.multiple_of(piece * width, width)
        out[node, :, pl.ds(start, width)] = acc[item] + end_recv[place]

    steps = items // GROUP
    slots = GROUP * (steps + GROUP - 1)

    def place_of(slot):
        part = slot % GROUP
        step = slot // GROUP - part
        item = (step // nodes * GROUP + part) * nodes + step % nodes
        return (slot >= 0) & (step >= 0) & (step < steps), item

    def tick(time, _):
        step = time // GROUP

        @pl.when((time % GROUP == 0) & (step < steps) & (step % nodes == 0))
        def _():
            local(step // nodes)

        @pl.when((time % GROUP == 0) & (step < steps))
        def _():
            first(step)

        for hop in range(1, hops):
            slot = time - LAGS[0] - (hop - 1) * LAGS[1]
            held, item = place_of(slot)

            @pl.when(held)
            def _():
                if hop == hops - 1:
                    last(item, slot == 0)
                else:
                    middle(hop, item, slot == 0)

        slot = time - LAGS[0] - (hops - 2) * LAGS[1] - LAGS[2]
        held, item = place_of(slot)

        @pl.when(held & ((item // nodes) % cols == cols - 1))
        def _():
            finish(item)

        return 0

    lax.fori_loop(0, slots + LAGS[0] + (hops - 2) * LAGS[1] + LAGS[2], tick, 0)

    def drain_hops(item, _):
        for hop in range(hops - 1):
            hop_copy(hop, item).wait_send()
        return 0

    def drain_cols(item, _):
        col_copy(item).wait_send()
        return 0

    def drain_end(place, _):
        end_copy(place).wait_send()
        return 0

    lax.fori_loop(0, items, drain_hops, 0)
    lax.fori_loop(0, theirs, drain_cols, 0)
    lax.fori_loop(0, items - theirs, drain_end, 0)


def shards(cols, coefficients, self_weights, cross_weights, true_ranks):
    nodes, rank, illum = coefficients.shape[1:]
    levels = self_weights.shape[1]
    shard = illum // cols
    width = min(WIDTH, shard)
    items = illum // width * nodes
    mine = shard // width * nodes
    theirs = items - mine
    hops = levels - (nodes.bit_length() - 1)
    tile = (rank, width)
    dma = pltpu.SemaphoreType.DMA
    return pl.pallas_call(
        functools.partial(kernel, cols, nodes, levels, width, shard),
        out_shape=jax.ShapeDtypeStruct((nodes, rank, shard), jnp.float32),
        in_specs=[pl.BlockSpec(memory_space=pl.ANY)] * 3 + [pl.BlockSpec(memory_space=pltpu.SMEM)],
        out_specs=pl.BlockSpec(memory_space=pltpu.VMEM),
        scratch_shapes=[
            pltpu.VMEM((items, *tile), jnp.float32),
            pltpu.VMEM((GROUP, nodes, *tile), jnp.float32),
            pltpu.VMEM((levels, nodes, rank, rank), jnp.bfloat16),
            pltpu.VMEM((levels, nodes, rank, rank), jnp.bfloat16),
            pltpu.VMEM((hops - 1, items, *tile), jnp.float32),
            pltpu.VMEM((hops - 1, items, *tile), jnp.float32),
            pltpu.VMEM((theirs, 2, *tile), jnp.float32),
            pltpu.VMEM((theirs, 2, *tile), jnp.float32),
            pltpu.VMEM((mine, *tile), jnp.float32),
            pltpu.VMEM((mine, *tile), jnp.float32),
            pltpu.VMEM((nodes, 8, width), jnp.int32),
            pltpu.VMEM((nodes, 8, width), jnp.int32),
            dma((items // nodes,)),
            dma((2, levels)),
            dma((hops - 1, items)),
            dma((hops - 1, items)),
            dma((theirs,)),
            dma((theirs,)),
            dma((mine,)),
            dma((mine,)),
            dma((2,)),
        ],
        compiler_params=pltpu.CompilerParams(
            collective_id=0, has_side_effects=True, vmem_limit_bytes=51 * 1024 * 1024
        ),
    )(coefficients, self_weights, cross_weights, true_ranks)


def solution(mesh):
    placed = (
        P("col", "node", None, None),
        P("col", None, "node", None, None),
        P("col", None, "node", None, None),
        P("col", "node"),
    )
    return jax.shard_map(
        functools.partial(shards, mesh.shape["col"]),
        mesh=mesh, in_specs=placed, out_specs=P("node", None, "col"), check_vma=False,
    )
```

```python
import functools

import jax
import jax.numpy as jnp
from jax import lax
from jax.experimental import pallas as pl
from jax.experimental.pallas import tpu as pltpu
from jax.sharding import PartitionSpec as P

WIDTH = 128
GROUP = 2
LAGS = (1, 3, 4, 16)


def flip(index, mask):
    return index + mask * (1 - 2 * ((index // mask) % 2))


def split(state):
    high = state.astype(jnp.bfloat16)
    low = (state - high.astype(jnp.float32)).astype(jnp.bfloat16)
    return high, low


def product(weights, parts):
    high, low = parts
    return jnp.dot(weights, high, preferred_element_type=jnp.float32) + jnp.dot(
        weights, low, preferred_element_type=jnp.float32
    )


def kernel(
    cols, nodes, levels, width, shard,
    coeff, self_hbm, cross_hbm, ranks_hbm, out,
    acc, tmp, self_w, cross_w, send, recv, col_send, col_recv, end_send, end_recv,
    ranks, own_rank, other_rank,
    load_sem, weight_sem, send_sem, recv_sem, col_send_sem, col_recv_sem,
    end_send_sem, end_recv_sem, rank_sem, rank_load_sem,
):
    rank_rows = acc.shape[1]
    local_bits = nodes.bit_length() - 1
    hops = levels - local_bits
    pieces = shard // width
    chunks = cols * pieces
    items = chunks * nodes
    theirs = (cols - 1) * pieces * nodes
    me = lax.axis_index("node")
    my_col = lax.axis_index("col")
    peers = [flip(me, 1 << hop) for hop in range(hops)]

    def load(chunk):
        column = (my_col + 1 + chunk % cols) % cols
        start = pl.multiple_of(column * shard + (chunk // cols) * width, width)
        return pltpu.make_async_copy(
            coeff.at[0, :, :, pl.ds(start, width)],
            acc.at[pl.ds(chunk * nodes, nodes)],
            load_sem.at[chunk],
        )

    def weight_loads(level):
        return (
            pltpu.make_async_copy(self_hbm.at[0, level], self_w.at[level], weight_sem.at[0, level]),
            pltpu.make_async_copy(cross_hbm.at[0, level], cross_w.at[level], weight_sem.at[1, level]),
        )

    def hop_copy(hop, item):
        return pltpu.make_async_remote_copy(
            src_ref=send.at[hop, item],
            dst_ref=recv.at[hop, item],
            send_sem=send_sem.at[hop, item],
            recv_sem=recv_sem.at[hop, item],
            device_id={"node": peers[hop]},
            device_id_type=pl.DeviceIdType.MESH,
        )

    def col_copy(item):
        column = (my_col + 1 + (item // nodes) % (cols - 1)) % cols
        return pltpu.make_async_remote_copy(
            src_ref=col_send.at[item],
            dst_ref=col_recv.at[item],
            send_sem=col_send_sem.at[item],
            recv_sem=col_recv_sem.at[item],
            device_id={"col": column},
            device_id_type=pl.DeviceIdType.MESH,
        )

    def end_copy(place):
        return pltpu.make_async_remote_copy(
            src_ref=end_send.at[place],
            dst_ref=end_recv.at[place],
            send_sem=end_send_sem.at[place],
            recv_sem=end_recv_sem.at[place],
            device_id={"node": peers[hops - 1]},
            device_id_type=pl.DeviceIdType.MESH,
        )

    rank_copy = pltpu.make_async_remote_copy(
        src_ref=own_rank,
        dst_ref=other_rank,
        send_sem=rank_sem.at[0],
        recv_sem=rank_sem.at[1],
        device_id={"node": peers[hops - 1]},
        device_id_type=pl.DeviceIdType.MESH,
    )

    rank_load = pltpu.make_async_copy(ranks_hbm, ranks, rank_load_sem)
    rank_load.start()
    for chunk in range(GROUP):
        load(chunk).start()
    for copy in weight_loads(0):
        copy.start()

    barrier = pltpu.get_barrier_semaphore()
    for peer in peers:
        pl.semaphore_signal(barrier, inc=1, device_id={"node": peer}, device_id_type=pl.DeviceIdType.MESH)
    for step in range(1, cols):
        pl.semaphore_signal(
            barrier, inc=1, device_id={"col": (my_col + step) % cols}, device_id_type=pl.DeviceIdType.MESH
        )
    rank_load.wait()
    for level in range(1, local_bits + 1):
        for copy in weight_loads(level):
            copy.start()
    for node in range(nodes):
        own_rank[node] = jnp.full(own_rank.shape[1:], ranks[0, node], jnp.int32)

    row = lax.broadcasted_iota(jnp.int32, (rank_rows, width), 0)

    def masked(values, rank_tile):
        return jnp.where(row < rank_tile[0:1, :], values, 0.0)

    def state(bank, chunk, node):
        return acc.at[chunk * nodes + node] if bank == 0 else tmp.at[chunk % GROUP, node]

    def stack(bank, pair, node, parts):
        halves = [split(state(bank, pair * GROUP + part, node)[...]) for part in parts]
        return tuple(jnp.concatenate(half, axis=1) for half in zip(*halves))

    def wide(weights, both):
        value = jnp.dot(weights, both, preferred_element_type=jnp.float32)
        return value[:, :width] + value[:, width:]

    def times(weights, stacked):
        if stacked[0].shape[1] == width:
            return wide(weights, jnp.concatenate(stacked, axis=1))
        return product(weights, stacked)

    def columns(values, at):
        return values[:, at * width : (at + 1) * width]

    def local(pair, parts, fresh):
        for part in parts:
            load(pair * GROUP + part).wait()
        for level in range(local_bits):
            if fresh:
                for copy in weight_loads(level):
                    copy.wait()
            for node in range(nodes):
                other = node + (1 << level)
                if (node >> level) % 2:
                    continue
                mine, theirs = stack(level % 2, pair, node, parts), stack(level % 2, pair, other, parts)
                for to, at, source in ((node, mine, theirs), (other, theirs, mine)):
                    value = times(self_w[level, to], at)
                    value += times(cross_w[level, node + other - to], source)
                    for index, part in enumerate(parts):
                        state((level + 1) % 2, pair * GROUP + part, to)[...] = masked(
                            columns(value, index), own_rank[to]
                        )

    def first(step, parts):
        pair, node = step // nodes, step % nodes
        stacked = stack(local_bits % 2, pair, node, parts)
        value = times(cross_w[local_bits, node], stacked)
        for index, part in enumerate(parts):
            send[0, (pair * GROUP + part) * nodes + node] = columns(value, index)
            hop_copy(0, (pair * GROUP + part) * nodes + node).start()
        value = times(self_w[local_bits, node], stacked)
        for index, part in enumerate(parts):
            acc[(pair * GROUP + part) * nodes + node] = columns(value, index)

    def combine(hop, item, lead):
        level = local_bits + hop

        @pl.when(lead)
        def _():
            for copy in weight_loads(level):
                copy.wait()

        hop_copy(hop - 1, item).wait_recv()
        node = item % nodes
        high, low = split(masked(acc[item] + recv[hop - 1, item], own_rank[node]))
        return node, level, jnp.concatenate([high, low], axis=1)

    def middle(hop, item, lead):
        node, level, parts = combine(hop, item, lead)
        send[hop, item] = wide(cross_w[level, node], parts)
        hop_copy(hop, item).start()
        acc[item] = wide(self_w[level, node], parts)

    def last(item, lead):
        node, level, parts = combine(hops - 1, item, lead)

        @pl.when(lead)
        def _():
            rank_copy.wait()

        sent = masked(wide(cross_w[level, node], parts), other_rank[node])
        kept = masked(wide(self_w[level, node], parts), own_rank[node])

        chunk = item // nodes
        piece = chunk // cols

        @pl.when(chunk % cols < cols - 1)
        def _():
            slot = (piece * (cols - 1) + chunk % cols) * nodes + node
            col_send[slot, 0] = kept
            col_send[slot, 1] = sent
            col_copy(slot).start()

        @pl.when(chunk % cols == cols - 1)
        def _():
            place = piece * nodes + node
            total_kept, total_sent = kept, sent
            for step in range(cols - 1):
                slot = (piece * (cols - 1) + step) * nodes + node
                col_copy(slot).wait_recv()
                total_kept += col_recv[slot, 0]
                total_sent += col_recv[slot, 1]
            end_send[place] = total_sent
            end_copy(place).start()
            acc[item] = total_kept

    def finish(item):
        node = item % nodes
        piece = item // (nodes * cols)
        place = piece * nodes + node
        end_copy(place).wait()
        start = pl.multiple_of(piece * width, width)
        out[node, :, pl.ds(start, width)] = acc[item] + end_recv[place]

    steps = items // GROUP
    slots = GROUP * (steps + GROUP - 1)

    def lag(hop):
        return LAGS[0] + (min(hop, hops - 2) - 1) * LAGS[1] + sum(LAGS[2 : 4 + hop - hops])

    def place_of(slot):
        part = slot % GROUP
        step = slot // GROUP - part
        item = (step // nodes * GROUP + part) * nodes + step % nodes
        return (slot >= 0) & (step >= 0) & (step < steps), item

    local(0, (0,), True)
    for level in range(local_bits + 1, levels):
        for copy in weight_loads(level):
            copy.start()
    for copy in weight_loads(local_bits):
        copy.wait()
    pl.semaphore_wait(barrier, hops + cols - 1)
    rank_copy.start()
    first(0, (0,))
    for chunk in range(GROUP, chunks):
        load(chunk).start()
    for part in range(1, GROUP):
        local(0, (part,), False)
        first(0, (part,))

    def tick(time, _):
        step = time // GROUP

        @pl.when((time % GROUP == 0) & (step > 0) & (step < steps) & (step % nodes == 0))
        def _():
            local(step // nodes, tuple(range(GROUP)), False)

        @pl.when((time % GROUP == 0) & (step > 0) & (step < steps))
        def _():
            first(step, tuple(range(GROUP)))

        for hop in range(1, hops):
            slot = time - lag(hop)
            held, item = place_of(slot)

            @pl.when(held)
            def _():
                if hop == hops - 1:
                    last(item, slot == 0)
                else:
                    middle(hop, item, slot == 0)

        slot = time - lag(hops)
        held, item = place_of(slot)

        chunk = item // nodes

        @pl.when(held)
        def _():
            for hop in range(hops - 1):
                hop_copy(hop, item).wait_send()

        @pl.when(held & (chunk % cols < cols - 1))
        def _():
            col_copy((chunk // cols * (cols - 1) + chunk % cols) * nodes + item % nodes).wait_send()

        @pl.when(held & (chunk % cols == cols - 1))
        def _():
            finish(item)

        return 0

    lax.fori_loop(0, slots + lag(hops), tick, 0)


def shards(cols, coefficients, self_weights, cross_weights, true_ranks):
    nodes, rank, illum = coefficients.shape[1:]
    levels = self_weights.shape[1]
    shard = illum // cols
    width = min(WIDTH, shard)
    items = illum // width * nodes
    mine = shard // width * nodes
    theirs = items - mine
    hops = levels - (nodes.bit_length() - 1)
    tile = (rank, width)
    dma = pltpu.SemaphoreType.DMA
    return pl.pallas_call(
        functools.partial(kernel, cols, nodes, levels, width, shard),
        out_shape=jax.ShapeDtypeStruct((nodes, rank, shard), jnp.float32),
        in_specs=[pl.BlockSpec(memory_space=pl.ANY)] * 3 + [pl.BlockSpec(memory_space=pltpu.HBM)],
        out_specs=pl.BlockSpec(memory_space=pltpu.VMEM),
        scratch_shapes=[
            pltpu.VMEM((items, *tile), jnp.float32),
            pltpu.VMEM((GROUP, nodes, *tile), jnp.float32),
            pltpu.VMEM((levels, nodes, rank, rank), jnp.bfloat16),
            pltpu.VMEM((levels, nodes, rank, rank), jnp.bfloat16),
            pltpu.VMEM((hops - 1, items, *tile), jnp.float32),
            pltpu.VMEM((hops - 1, items, *tile), jnp.float32),
            pltpu.VMEM((theirs, 2, *tile), jnp.float32),
            pltpu.VMEM((theirs, 2, *tile), jnp.float32),
            pltpu.VMEM((mine, *tile), jnp.float32),
            pltpu.VMEM((mine, *tile), jnp.float32),
            pltpu.SMEM(true_ranks.shape, jnp.int32),
            pltpu.VMEM((nodes, 8, width), jnp.int32),
            pltpu.VMEM((nodes, 8, width), jnp.int32),
            dma((items // nodes,)),
            dma((2, levels)),
            dma((hops - 1, items)),
            dma((hops - 1, items)),
            dma((theirs,)),
            dma((theirs,)),
            dma((mine,)),
            dma((mine,)),
            dma((2,)),
            dma,
        ],
        compiler_params=pltpu.CompilerParams(
            collective_id=0, has_side_effects=True, vmem_limit_bytes=51 * 1024 * 1024
        ),
    )(coefficients, self_weights, cross_weights, pltpu.with_memory_space_constraint(true_ranks, pltpu.HBM))


def solution(mesh):
    placed = (
        P("col", "node", None, None),
        P("col", None, "node", None, None),
        P("col", None, "node", None, None),
        P("col", "node"),
    )
    return jax.shard_map(
        functools.partial(shards, mesh.shape["col"]),
        mesh=mesh, in_specs=placed, out_specs=P("node", None, "col"), check_vma=False,
    )
```

```python
import functools

import jax
import jax.numpy as jnp
from jax import lax
from jax.experimental import pallas as pl
from jax.experimental.pallas import tpu as pltpu
from jax.sharding import PartitionSpec as P

WIDTH = 128
GROUP = 2
RING = 16
LAGS = (1, 3, 4, 16)


def flip(index, mask):
    return index + mask * (1 - 2 * ((index // mask) % 2))


def split(state):
    high = state.astype(jnp.bfloat16)
    low = (state - high.astype(jnp.float32)).astype(jnp.bfloat16)
    return high, low


def product(weights, parts):
    high, low = parts
    return jnp.dot(weights, high, preferred_element_type=jnp.float32) + jnp.dot(
        weights, low, preferred_element_type=jnp.float32
    )


def kernel(
    cols, nodes, levels, width, shard,
    coeff, self_hbm, cross_hbm, ranks_hbm, out,
    acc, tmp, self_w, cross_w, send, recv, col_send, col_recv, end_send, end_recv,
    ranks, own_rank, other_rank,
    load_sem, weight_sem, send_sem, recv_sem, col_send_sem, col_recv_sem,
    end_send_sem, end_recv_sem, rank_sem, rank_load_sem,
):
    rank_rows = acc.shape[1]
    local_bits = nodes.bit_length() - 1
    hops = levels - local_bits
    pieces = shard // width
    chunks = cols * pieces
    items = chunks * nodes
    theirs = (cols - 1) * pieces * nodes
    me = lax.axis_index("node")
    my_col = lax.axis_index("col")
    peers = [flip(me, 1 << hop) for hop in range(hops)]

    def load(chunk):
        column = (my_col + 1 + chunk % cols) % cols
        start = pl.multiple_of(column * shard + (chunk // cols) * width, width)
        return pltpu.make_async_copy(
            coeff.at[0, :, :, pl.ds(start, width)],
            acc.at[pl.ds(chunk * nodes, nodes)],
            load_sem.at[chunk],
        )

    def weight_loads(level):
        return (
            pltpu.make_async_copy(self_hbm.at[0, level], self_w.at[level], weight_sem.at[0, level]),
            pltpu.make_async_copy(cross_hbm.at[0, level], cross_w.at[level], weight_sem.at[1, level]),
        )

    def ring(item):
        chunk = item // nodes
        part = chunk % GROUP
        return (GROUP * (chunk // GROUP * nodes + item % nodes + part) + part) % RING

    def hop_copy(hop, item):
        return pltpu.make_async_remote_copy(
            src_ref=send.at[hop, item],
            dst_ref=recv.at[hop, item],
            send_sem=send_sem.at[hop],
            recv_sem=recv_sem.at[hop, ring(item)],
            device_id={"node": peers[hop]},
            device_id_type=pl.DeviceIdType.MESH,
        )

    def whole_copy(source, target, source_sem, target_sem):
        return pltpu.make_async_remote_copy(
            src_ref=source,
            dst_ref=target,
            send_sem=source_sem,
            recv_sem=target_sem,
            device_id={"node": peers[0]},
            device_id_type=pl.DeviceIdType.MESH,
        )

    def col_copy(item):
        column = (my_col + 1 + (item // nodes) % (cols - 1)) % cols
        return pltpu.make_async_remote_copy(
            src_ref=col_send.at[item],
            dst_ref=col_recv.at[item],
            send_sem=col_send_sem,
            recv_sem=col_recv_sem.at[item],
            device_id={"col": column},
            device_id_type=pl.DeviceIdType.MESH,
        )

    def end_copy(place):
        return pltpu.make_async_remote_copy(
            src_ref=end_send.at[place],
            dst_ref=end_recv.at[place],
            send_sem=end_send_sem,
            recv_sem=end_recv_sem.at[place],
            device_id={"node": peers[hops - 1]},
            device_id_type=pl.DeviceIdType.MESH,
        )

    rank_copy = pltpu.make_async_remote_copy(
        src_ref=own_rank,
        dst_ref=other_rank,
        send_sem=rank_sem.at[0],
        recv_sem=rank_sem.at[1],
        device_id={"node": peers[hops - 1]},
        device_id_type=pl.DeviceIdType.MESH,
    )

    rank_load = pltpu.make_async_copy(ranks_hbm, ranks, rank_load_sem)
    rank_load.start()
    for chunk in range(GROUP):
        load(chunk).start()
    for copy in weight_loads(0):
        copy.start()

    barrier = pltpu.get_barrier_semaphore()
    for peer in peers:
        pl.semaphore_signal(barrier, inc=1, device_id={"node": peer}, device_id_type=pl.DeviceIdType.MESH)
    for step in range(1, cols):
        pl.semaphore_signal(
            barrier, inc=1, device_id={"col": (my_col + step) % cols}, device_id_type=pl.DeviceIdType.MESH
        )
    rank_load.wait()
    for level in range(1, local_bits + 1):
        for copy in weight_loads(level):
            copy.start()
    for node in range(nodes):
        own_rank[node] = jnp.full(own_rank.shape[1:], ranks[0, node], jnp.int32)

    row = lax.broadcasted_iota(jnp.int32, (rank_rows, width), 0)

    def masked(values, rank_tile):
        return jnp.where(row < rank_tile[0:1, :], values, 0.0)

    def state(bank, chunk, node):
        return acc.at[chunk * nodes + node] if bank == 0 else tmp.at[chunk % GROUP, node]

    def stack(bank, pair, node, parts):
        halves = [split(state(bank, pair * GROUP + part, node)[...]) for part in parts]
        return tuple(jnp.concatenate(half, axis=1) for half in zip(*halves))

    def wide(weights, both):
        value = jnp.dot(weights, both, preferred_element_type=jnp.float32)
        return value[:, :width] + value[:, width:]

    def times(weights, stacked):
        if stacked[0].shape[1] == width:
            return wide(weights, jnp.concatenate(stacked, axis=1))
        return product(weights, stacked)

    def columns(values, at):
        return values[:, at * width : (at + 1) * width]

    def local(pair, parts, fresh):
        for part in parts:
            load(pair * GROUP + part).wait()
        for level in range(local_bits):
            if fresh:
                for copy in weight_loads(level):
                    copy.wait()
            for node in range(nodes):
                other = node + (1 << level)
                if (node >> level) % 2:
                    continue
                mine, theirs = stack(level % 2, pair, node, parts), stack(level % 2, pair, other, parts)
                for to, at, source in ((node, mine, theirs), (other, theirs, mine)):
                    value = times(self_w[level, to], at)
                    value += times(cross_w[level, node + other - to], source)
                    for index, part in enumerate(parts):
                        state((level + 1) % 2, pair * GROUP + part, to)[...] = masked(
                            columns(value, index), own_rank[to]
                        )

    def first(step, parts):
        pair, node = step // nodes, step % nodes
        stacked = stack(local_bits % 2, pair, node, parts)
        value = times(cross_w[local_bits, node], stacked)
        for index, part in enumerate(parts):
            send[0, (pair * GROUP + part) * nodes + node] = columns(value, index)
            hop_copy(0, (pair * GROUP + part) * nodes + node).start()
        value = times(self_w[local_bits, node], stacked)
        for index, part in enumerate(parts):
            acc[(pair * GROUP + part) * nodes + node] = columns(value, index)

    def combine(hop, item, lead):
        level = local_bits + hop

        @pl.when(lead)
        def _():
            for copy in weight_loads(level):
                copy.wait()

        hop_copy(hop - 1, item).wait_recv()
        node = item % nodes
        high, low = split(masked(acc[item] + recv[hop - 1, item], own_rank[node]))
        return node, level, jnp.concatenate([high, low], axis=1)

    def middle(hop, item, lead):
        node, level, parts = combine(hop, item, lead)
        send[hop, item] = wide(cross_w[level, node], parts)
        hop_copy(hop, item).start()
        acc[item] = wide(self_w[level, node], parts)

    def last(item, lead):
        node, level, parts = combine(hops - 1, item, lead)

        @pl.when(lead)
        def _():
            rank_copy.wait()

        sent = masked(wide(cross_w[level, node], parts), other_rank[node])
        kept = masked(wide(self_w[level, node], parts), own_rank[node])

        chunk = item // nodes
        piece = chunk // cols

        @pl.when(chunk % cols < cols - 1)
        def _():
            slot = (piece * (cols - 1) + chunk % cols) * nodes + node
            col_send[slot, 0] = kept
            col_send[slot, 1] = sent
            col_copy(slot).start()

        @pl.when(chunk % cols == cols - 1)
        def _():
            place = piece * nodes + node
            total_kept, total_sent = kept, sent
            for step in range(cols - 1):
                slot = (piece * (cols - 1) + step) * nodes + node
                col_copy(slot).wait_recv()
                total_kept += col_recv[slot, 0]
                total_sent += col_recv[slot, 1]
            end_send[place] = total_sent
            end_copy(place).start()
            acc[item] = total_kept

    def finish(item):
        node = item % nodes
        piece = item // (nodes * cols)
        place = piece * nodes + node
        end_copy(place).wait_recv()
        start = pl.multiple_of(piece * width, width)
        out[node, :, pl.ds(start, width)] = acc[item] + end_recv[place]

    steps = items // GROUP
    slots = GROUP * (steps + GROUP - 1)

    def lag(hop):
        return LAGS[0] + (min(hop, hops - 2) - 1) * LAGS[1] + sum(LAGS[2 : 4 + hop - hops])

    def place_of(slot):
        part = slot % GROUP
        step = slot // GROUP - part
        item = (step // nodes * GROUP + part) * nodes + step % nodes
        return (slot >= 0) & (step >= 0) & (step < steps), item

    local(0, (0,), True)
    for level in range(local_bits + 1, levels):
        for copy in weight_loads(level):
            copy.start()
    for copy in weight_loads(local_bits):
        copy.wait()
    pl.semaphore_wait(barrier, hops + cols - 1)
    rank_copy.start()
    first(0, (0,))
    for chunk in range(GROUP, chunks):
        load(chunk).start()
    for part in range(1, GROUP):
        local(0, (part,), False)
        first(0, (part,))

    def tick(time, _):
        step = time // GROUP

        @pl.when((time % GROUP == 0) & (step > 0) & (step < steps) & (step % nodes == 0))
        def _():
            local(step // nodes, tuple(range(GROUP)), False)

        @pl.when((time % GROUP == 0) & (step > 0) & (step < steps))
        def _():
            first(step, tuple(range(GROUP)))

        for hop in range(1, hops):
            slot = time - lag(hop)
            held, item = place_of(slot)

            @pl.when(held)
            def _():
                if hop == hops - 1:
                    last(item, slot == 0)
                else:
                    middle(hop, item, slot == 0)

        slot = time - lag(hops)
        held, item = place_of(slot)

        @pl.when(held & ((item // nodes) % cols == cols - 1))
        def _():
            finish(item)

        return 0

    lax.fori_loop(0, slots + lag(hops), tick, 0)

    for hop in range(hops - 1):
        whole_copy(send.at[hop], recv.at[hop], send_sem.at[hop], recv_sem.at[hop, 0]).wait_send()
    whole_copy(col_send, col_recv, col_send_sem, col_recv_sem.at[0]).wait_send()
    whole_copy(end_send, end_recv, end_send_sem, end_recv_sem.at[0]).wait_send()


def shards(cols, coefficients, self_weights, cross_weights, true_ranks):
    nodes, rank, illum = coefficients.shape[1:]
    levels = self_weights.shape[1]
    shard = illum // cols
    width = min(WIDTH, shard)
    items = illum // width * nodes
    mine = shard // width * nodes
    theirs = items - mine
    hops = levels - (nodes.bit_length() - 1)
    tile = (rank, width)
    dma = pltpu.SemaphoreType.DMA
    return pl.pallas_call(
        functools.partial(kernel, cols, nodes, levels, width, shard),
        out_shape=jax.ShapeDtypeStruct((nodes, rank, shard), jnp.float32),
        in_specs=[pl.BlockSpec(memory_space=pl.ANY)] * 3 + [pl.BlockSpec(memory_space=pltpu.HBM)],
        out_specs=pl.BlockSpec(memory_space=pltpu.VMEM),
        scratch_shapes=[
            pltpu.VMEM((items, *tile), jnp.float32),
            pltpu.VMEM((GROUP, nodes, *tile), jnp.float32),
            pltpu.VMEM((levels, nodes, rank, rank), jnp.bfloat16),
            pltpu.VMEM((levels, nodes, rank, rank), jnp.bfloat16),
            pltpu.VMEM((hops - 1, items, *tile), jnp.float32),
            pltpu.VMEM((hops - 1, items, *tile), jnp.float32),
            pltpu.VMEM((theirs, 2, *tile), jnp.float32),
            pltpu.VMEM((theirs, 2, *tile), jnp.float32),
            pltpu.VMEM((mine, *tile), jnp.float32),
            pltpu.VMEM((mine, *tile), jnp.float32),
            pltpu.SMEM(true_ranks.shape, jnp.int32),
            pltpu.VMEM((nodes, 8, width), jnp.int32),
            pltpu.VMEM((nodes, 8, width), jnp.int32),
            dma((items // nodes,)),
            dma((2, levels)),
            dma((hops - 1,)),
            dma((hops - 1, RING)),
            dma,
            dma((theirs,)),
            dma,
            dma((mine,)),
            dma((2,)),
            dma,
        ],
        compiler_params=pltpu.CompilerParams(
            collective_id=0, has_side_effects=True, vmem_limit_bytes=51 * 1024 * 1024
        ),
    )(coefficients, self_weights, cross_weights, pltpu.with_memory_space_constraint(true_ranks, pltpu.HBM))


def solution(mesh):
    placed = (
        P("col", "node", None, None),
        P("col", None, "node", None, None),
        P("col", None, "node", None, None),
        P("col", "node"),
    )
    return jax.shard_map(
        functools.partial(shards, mesh.shape["col"]),
        mesh=mesh, in_specs=placed, out_specs=P("node", None, "col"), check_vma=False,
    )
```

```python
import functools

import jax
import jax.numpy as jnp
from jax import lax
from jax.experimental import pallas as pl
from jax.experimental.pallas import tpu as pltpu
from jax.sharding import PartitionSpec as P

WIDTH = 128
GROUP = 2
RING = 12
COL_RING = 8
LAGS = (1, 3, 4, 16)


def flip(index, mask):
    return index + mask * (1 - 2 * ((index // mask) % 2))


def split(state):
    high = state.astype(jnp.bfloat16)
    low = (state - high.astype(jnp.float32)).astype(jnp.bfloat16)
    return high, low


def product(weights, parts):
    high, low = parts
    return jnp.dot(weights, high, preferred_element_type=jnp.float32) + jnp.dot(
        weights, low, preferred_element_type=jnp.float32
    )


def kernel(
    cols, nodes, levels, width, shard,
    coeff, self_hbm, cross_hbm, ranks_hbm, out,
    acc, tmp, self_w, cross_w, send, recv, col_send, col_recv, end_send, end_recv,
    ranks, own_rank, other_rank,
    load_sem, weight_sem, send_sem, recv_sem, col_send_sem, col_recv_sem,
    end_send_sem, end_recv_sem, rank_sem, rank_load_sem,
):
    rank_rows = acc.shape[1]
    local_bits = nodes.bit_length() - 1
    hops = levels - local_bits
    pieces = shard // width
    chunks = cols * pieces
    items = chunks * nodes
    theirs = (cols - 1) * pieces * nodes
    me = lax.axis_index("node")
    my_col = lax.axis_index("col")
    peers = [flip(me, 1 << hop) for hop in range(hops)]

    def load(chunk):
        column = (my_col + 1 + chunk % cols) % cols
        start = pl.multiple_of(column * shard + (chunk // cols) * width, width)
        return pltpu.make_async_copy(
            coeff.at[0, :, :, pl.ds(start, width)],
            acc.at[pl.ds(chunk * nodes, nodes)],
            load_sem.at[min(chunk, GROUP)],
        )

    bands = [(level, level + 1) for level in range(local_bits + 2)] + [(local_bits + 2, levels)]

    def weight_loads(group):
        band = pl.ds(bands[group][0], bands[group][1] - bands[group][0])
        return (
            pltpu.make_async_copy(self_hbm.at[0, band], self_w.at[band], weight_sem.at[0, group]),
            pltpu.make_async_copy(cross_hbm.at[0, band], cross_w.at[band], weight_sem.at[1, group]),
        )

    def ring(item):
        chunk = item // nodes
        part = chunk % GROUP
        return (GROUP * (chunk // GROUP * nodes + item % nodes + part) + part) % RING

    def hop_copy(hop, item):
        return pltpu.make_async_remote_copy(
            src_ref=send.at[hop, item],
            dst_ref=recv.at[hop, item],
            send_sem=send_sem.at[hop],
            recv_sem=recv_sem.at[hop, ring(item)],
            device_id={"node": peers[hop]},
            device_id_type=pl.DeviceIdType.MESH,
        )

    def whole_copy(source, target, source_sem, target_sem):
        return pltpu.make_async_remote_copy(
            src_ref=source,
            dst_ref=target,
            send_sem=source_sem,
            recv_sem=target_sem,
            device_id={"node": peers[0]},
            device_id_type=pl.DeviceIdType.MESH,
        )

    def col_copy(item):
        column = (my_col + 1 + (item // nodes) % (cols - 1)) % cols
        return pltpu.make_async_remote_copy(
            src_ref=col_send.at[item],
            dst_ref=col_recv.at[item],
            send_sem=col_send_sem,
            recv_sem=col_recv_sem.at[item // nodes % (cols - 1), (item // nodes // (cols - 1) * nodes + item % nodes) % col_recv_sem.shape[1]],
            device_id={"col": column},
            device_id_type=pl.DeviceIdType.MESH,
        )

    def end_copy(place):
        return pltpu.make_async_remote_copy(
            src_ref=end_send.at[place],
            dst_ref=end_recv.at[place],
            send_sem=end_send_sem,
            recv_sem=end_recv_sem.at[place],
            device_id={"node": peers[hops - 1]},
            device_id_type=pl.DeviceIdType.MESH,
        )

    rank_copy = pltpu.make_async_remote_copy(
        src_ref=own_rank,
        dst_ref=other_rank,
        send_sem=rank_sem.at[0],
        recv_sem=rank_sem.at[1],
        device_id={"node": peers[hops - 1]},
        device_id_type=pl.DeviceIdType.MESH,
    )

    rank_load = pltpu.make_async_copy(ranks_hbm, ranks, rank_load_sem)
    rank_load.start()
    load(0).start()
    for copy in weight_loads(0):
        copy.start()

    barrier = pltpu.get_barrier_semaphore()
    for peer in peers:
        pl.semaphore_signal(barrier, inc=1, device_id={"node": peer}, device_id_type=pl.DeviceIdType.MESH)
    for step in range(1, cols):
        pl.semaphore_signal(
            barrier, inc=1, device_id={"col": (my_col + step) % cols}, device_id_type=pl.DeviceIdType.MESH
        )
    rank_load.wait()
    for group in range(1, local_bits + 1):
        for copy in weight_loads(group):
            copy.start()
    for part in range(1, GROUP):
        load(part).start()
    for node in range(nodes):
        own_rank[node] = jnp.full(own_rank.shape[1:], ranks[0, node], jnp.int32)

    row = lax.broadcasted_iota(jnp.int32, (rank_rows, width), 0)

    def masked(values, rank_tile):
        return jnp.where(row < rank_tile[0:1, :], values, 0.0)

    def state(bank, chunk, node):
        return acc.at[chunk * nodes + node] if bank == 0 else tmp.at[chunk % GROUP, node]

    def stack(bank, pair, node, parts):
        halves = [split(state(bank, pair * GROUP + part, node)[...]) for part in parts]
        return tuple(jnp.concatenate(half, axis=1) for half in zip(*halves))

    def wide(weights, both):
        value = jnp.dot(weights, both, preferred_element_type=jnp.float32)
        return value[:, :width] + value[:, width:]

    def times(weights, stacked):
        if stacked[0].shape[1] == width:
            return wide(weights, jnp.concatenate(stacked, axis=1))
        return product(weights, stacked)

    def columns(values, at):
        return values[:, at * width : (at + 1) * width]

    def lower(level):
        return [node for node in range(nodes) if (node >> level) % 2 == 0]

    every = [(level, lower(level)) for level in range(local_bits)]
    early = every[:-1] + [(local_bits - 1, [0])]
    late = [(local_bits - 1, lower(local_bits - 1)[1:])]

    def local(pair, parts, stages):
        for level, chosen in stages:
            for node in chosen:
                other = node + (1 << level)
                mine, theirs = stack(level % 2, pair, node, parts), stack(level % 2, pair, other, parts)
                for to, at, source in ((node, mine, theirs), (other, theirs, mine)):
                    value = times(self_w[level, to], at)
                    value += times(cross_w[level, node + other - to], source)
                    for index, part in enumerate(parts):
                        state((level + 1) % 2, pair * GROUP + part, to)[...] = masked(
                            columns(value, index), own_rank[to]
                        )

    def first(step, parts):
        pair, node = step // nodes, step % nodes
        stacked = stack(local_bits % 2, pair, node, parts)
        value = times(cross_w[local_bits, node], stacked)
        for index, part in enumerate(parts):
            send[0, (pair * GROUP + part) * nodes + node] = columns(value, index)
            hop_copy(0, (pair * GROUP + part) * nodes + node).start()
        value = times(self_w[local_bits, node], stacked)
        for index, part in enumerate(parts):
            acc[(pair * GROUP + part) * nodes + node] = columns(value, index)

    def combine(hop, item, lead):
        level = local_bits + hop

        if level < len(bands):

            @pl.when(lead)
            def _():
                for copy in weight_loads(level):
                    copy.wait()

        hop_copy(hop - 1, item).wait_recv()
        node = item % nodes
        high, low = split(masked(acc[item] + recv[hop - 1, item], own_rank[node]))
        return node, level, jnp.concatenate([high, low], axis=1)

    def middle(hop, item, lead):
        node, level, parts = combine(hop, item, lead)
        send[hop, item] = wide(cross_w[level, node], parts)
        hop_copy(hop, item).start()
        acc[item] = wide(self_w[level, node], parts)

    def last(item, lead):
        node, level, parts = combine(hops - 1, item, lead)

        @pl.when(lead)
        def _():
            rank_copy.wait()

        sent = masked(wide(cross_w[level, node], parts), other_rank[node])
        chunk = item // nodes
        piece = chunk // cols

        @pl.when(chunk % cols < cols - 1)
        def _():
            slot = (piece * (cols - 1) + chunk % cols) * nodes + node
            col_send[slot, 1] = sent
            col_send[slot, 0] = masked(wide(self_w[level, node], parts), own_rank[node])
            col_copy(slot).start()

        @pl.when(chunk % cols == cols - 1)
        def _():
            place = piece * nodes + node
            first_slot = piece * (cols - 1) * nodes + node
            total = sent
            for step in range(cols - 1):
                col_copy(first_slot + step * nodes).wait_recv()
                total += col_recv[first_slot + step * nodes, 1]
            end_send[place] = total
            end_copy(place).start()
            total = masked(wide(self_w[level, node], parts), own_rank[node])
            for step in range(cols - 1):
                total += col_recv[first_slot + step * nodes, 0]
            acc[item] = total

    def finish(item):
        node = item % nodes
        piece = item // (nodes * cols)
        place = piece * nodes + node
        end_copy(place).wait_recv()
        start = pl.multiple_of(piece * width, width)
        out[node, :, pl.ds(start, width)] = acc[item] + end_recv[place]

    steps = items // GROUP
    slots = GROUP * (steps + GROUP - 1)

    def lag(hop):
        return LAGS[0] + (min(hop, hops - 2) - 1) * LAGS[1] + sum(LAGS[2 : 4 + hop - hops])

    def place_of(slot):
        part = slot % GROUP
        step = slot // GROUP - part
        item = (step // nodes * GROUP + part) * nodes + step % nodes
        return (slot >= 0) & (step >= 0) & (step < steps), item

    load(0).wait()
    for level, chosen in early:
        for copy in weight_loads(level):
            copy.wait()
        local(0, (0,), [(level, chosen)])
    for group in range(local_bits + 1, len(bands)):
        for copy in weight_loads(group):
            copy.start()
    for copy in weight_loads(local_bits):
        copy.wait()
    pl.semaphore_wait(barrier, hops + cols - 1)
    rank_copy.start()
    first(0, (0,))
    for chunk in range(GROUP, chunks):
        load(chunk).start()
    local(0, (0,), late)
    def tick(time, _):
        step = time // GROUP

        @pl.when((time % GROUP == 0) & (step > 0) & (step < steps) & (step % nodes == 0))
        def _():
            @pl.when(step == nodes)
            def _():
                rest = pl.ds(GROUP * nodes, (chunks - GROUP) * nodes)
                pltpu.make_async_copy(acc.at[rest], acc.at[rest], load_sem.at[GROUP]).wait()

            local(step // nodes, tuple(range(GROUP)), every)

        @pl.when((time % GROUP == 0) & (step > 0) & (step < steps))
        def _():
            first(step, tuple(range(GROUP)))

        for hop in range(1, hops):
            slot = time - lag(hop)
            held, item = place_of(slot)

            @pl.when(held)
            def _():
                if hop == hops - 1:
                    last(item, slot == 0)
                else:
                    middle(hop, item, slot == 0)

        @pl.when(time == LAGS[0])
        def _():
            for part in range(1, GROUP):
                load(part).wait()
                local(0, (part,), every)
                first(0, (part,))

        slot = time - lag(hops)
        held, item = place_of(slot)

        @pl.when(held & ((item // nodes) % cols == cols - 1))
        def _():
            finish(item)

        return 0

    lax.fori_loop(0, slots + lag(hops), tick, 0)

    for hop in range(hops - 1):
        whole_copy(send.at[hop], recv.at[hop], send_sem.at[hop], recv_sem.at[hop, 0]).wait_send()
    whole_copy(col_send, col_recv, col_send_sem, col_recv_sem.at[0, 0]).wait_send()
    whole_copy(end_send, end_recv, end_send_sem, end_recv_sem.at[0]).wait_send()


def shards(cols, coefficients, self_weights, cross_weights, true_ranks):
    nodes, rank, illum = coefficients.shape[1:]
    levels = self_weights.shape[1]
    shard = illum // cols
    width = min(WIDTH, shard)
    items = illum // width * nodes
    mine = shard // width * nodes
    theirs = items - mine
    hops = levels - (nodes.bit_length() - 1)
    tile = (rank, width)
    dma = pltpu.SemaphoreType.DMA
    return pl.pallas_call(
        functools.partial(kernel, cols, nodes, levels, width, shard),
        out_shape=jax.ShapeDtypeStruct((nodes, rank, shard), jnp.float32),
        in_specs=[pl.BlockSpec(memory_space=pl.ANY)] * 3 + [pl.BlockSpec(memory_space=pltpu.HBM)],
        out_specs=pl.BlockSpec(memory_space=pltpu.VMEM),
        scratch_shapes=[
            pltpu.VMEM((items, *tile), jnp.float32),
            pltpu.VMEM((GROUP, nodes, *tile), jnp.float32),
            pltpu.VMEM((levels, nodes, rank, rank), jnp.bfloat16),
            pltpu.VMEM((levels, nodes, rank, rank), jnp.bfloat16),
            pltpu.VMEM((hops - 1, items, *tile), jnp.float32),
            pltpu.VMEM((hops - 1, items, *tile), jnp.float32),
            pltpu.VMEM((theirs, 2, *tile), jnp.float32),
            pltpu.VMEM((theirs, 2, *tile), jnp.float32),
            pltpu.VMEM((mine, *tile), jnp.float32),
            pltpu.VMEM((mine, *tile), jnp.float32),
            pltpu.SMEM(true_ranks.shape, jnp.int32),
            pltpu.VMEM((nodes, 8, width), jnp.int32),
            pltpu.VMEM((nodes, 8, width), jnp.int32),
            dma((GROUP + 1,)),
            dma((2, nodes.bit_length() + 2)),
            dma((hops - 1,)),
            dma((hops - 1, RING)),
            dma,
            dma((cols - 1, min(COL_RING, mine))),
            dma,
            dma((mine,)),
            dma((2,)),
            dma,
        ],
        compiler_params=pltpu.CompilerParams(
            collective_id=0, has_side_effects=True, vmem_limit_bytes=51 * 1024 * 1024
        ),
    )(coefficients, self_weights, cross_weights, pltpu.with_memory_space_constraint(true_ranks, pltpu.HBM))


def solution(mesh):
    placed = (
        P("col", "node", None, None),
        P("col", None, "node", None, None),
        P("col", None, "node", None, None),
        P("col", "node"),
    )
    return jax.shard_map(
        functools.partial(shards, mesh.shape["col"]),
        mesh=mesh, in_specs=placed, out_specs=P("node", None, "col"), check_vma=False,
    )
```

```python
import functools

import jax
import jax.numpy as jnp
from jax import lax
from jax.experimental import pallas as pl
from jax.experimental.pallas import tpu as pltpu
from jax.sharding import PartitionSpec as P

WIDTH = 128
GROUP = 2
RING = 12
COL_RING = 8
LAGS = (1, 3, 4, 16)


def flip(index, mask):
    return index + mask * (1 - 2 * ((index // mask) % 2))


def split(state):
    high = state.astype(jnp.bfloat16)
    low = (state - high.astype(jnp.float32)).astype(jnp.bfloat16)
    return high, low


def product(weights, parts):
    high, low = parts
    return jnp.dot(weights, high, preferred_element_type=jnp.float32) + jnp.dot(
        weights, low, preferred_element_type=jnp.float32
    )


def kernel(
    cols, nodes, levels, width, shard,
    coeff, self_hbm, cross_hbm, ranks_hbm, out,
    acc, tmp, self_w, cross_w, send, recv, col_send, col_recv, end_send, end_recv,
    tail_send, tail_recv, tail_keep,
    ranks, own_rank, other_rank,
    load_sem, weight_sem, send_sem, recv_sem, col_send_sem, col_recv_sem,
    end_send_sem, end_recv_sem, rank_sem, rank_load_sem, tail_sem,
):
    rank_rows = acc.shape[1]
    local_bits = nodes.bit_length() - 1
    hops = levels - local_bits
    pieces = shard // width
    chunks = cols * pieces
    items = chunks * nodes
    theirs = (cols - 1) * pieces * nodes
    me = lax.axis_index("node")
    my_col = lax.axis_index("col")
    peers = [flip(me, 1 << hop) for hop in range(hops)]

    def load(chunk):
        column = (my_col + 1 + chunk % cols) % cols
        start = pl.multiple_of(column * shard + (chunk // cols) * width, width)
        return pltpu.make_async_copy(
            coeff.at[0, :, :, pl.ds(start, width)],
            acc.at[pl.ds(chunk * nodes, nodes)],
            load_sem.at[min(chunk, GROUP)],
        )

    bands = [(level, level + 1) for level in range(local_bits + 2)] + [(local_bits + 2, levels)]

    def weight_loads(group):
        band = pl.ds(bands[group][0], bands[group][1] - bands[group][0])
        return (
            pltpu.make_async_copy(self_hbm.at[0, band], self_w.at[band], weight_sem.at[0, group]),
            pltpu.make_async_copy(cross_hbm.at[0, band], cross_w.at[band], weight_sem.at[1, group]),
        )

    def ring(item):
        chunk = item // nodes
        part = chunk % GROUP
        return (GROUP * (chunk // GROUP * nodes + item % nodes + part) + part) % RING

    def hop_copy(hop, item):
        return pltpu.make_async_remote_copy(
            src_ref=send.at[hop, item],
            dst_ref=recv.at[hop, item],
            send_sem=send_sem.at[hop],
            recv_sem=recv_sem.at[hop, ring(item)],
            device_id={"node": peers[hop]},
            device_id_type=pl.DeviceIdType.MESH,
        )

    def whole_copy(source, target, source_sem, target_sem):
        return pltpu.make_async_remote_copy(
            src_ref=source,
            dst_ref=target,
            send_sem=source_sem,
            recv_sem=target_sem,
            device_id={"node": peers[0]},
            device_id_type=pl.DeviceIdType.MESH,
        )

    def half_copy(stage, half):
        return pltpu.make_async_remote_copy(
            src_ref=tail_send.at[stage, half],
            dst_ref=tail_recv.at[stage, half],
            send_sem=tail_sem.at[0, stage, half],
            recv_sem=tail_sem.at[1, stage, half],
            device_id={"node": peers[hops - 2 + stage]},
            device_id_type=pl.DeviceIdType.MESH,
        )

    def col_copy(item):
        column = (my_col + 1 + (item // nodes) % (cols - 1)) % cols
        return pltpu.make_async_remote_copy(
            src_ref=col_send.at[item],
            dst_ref=col_recv.at[item],
            send_sem=col_send_sem,
            recv_sem=col_recv_sem.at[item // nodes % (cols - 1), (item // nodes // (cols - 1) * nodes + item % nodes) % col_recv_sem.shape[1]],
            device_id={"col": column},
            device_id_type=pl.DeviceIdType.MESH,
        )

    def end_copy(place):
        return pltpu.make_async_remote_copy(
            src_ref=end_send.at[place],
            dst_ref=end_recv.at[place],
            send_sem=end_send_sem,
            recv_sem=end_recv_sem.at[place],
            device_id={"node": peers[hops - 1]},
            device_id_type=pl.DeviceIdType.MESH,
        )

    rank_copy = pltpu.make_async_remote_copy(
        src_ref=own_rank,
        dst_ref=other_rank,
        send_sem=rank_sem.at[0],
        recv_sem=rank_sem.at[1],
        device_id={"node": peers[hops - 1]},
        device_id_type=pl.DeviceIdType.MESH,
    )

    rank_load = pltpu.make_async_copy(ranks_hbm, ranks, rank_load_sem)
    rank_load.start()
    load(0).start()
    for copy in weight_loads(0):
        copy.start()

    barrier = pltpu.get_barrier_semaphore()
    for peer in peers:
        pl.semaphore_signal(barrier, inc=1, device_id={"node": peer}, device_id_type=pl.DeviceIdType.MESH)
    for step in range(1, cols):
        pl.semaphore_signal(
            barrier, inc=1, device_id={"col": (my_col + step) % cols}, device_id_type=pl.DeviceIdType.MESH
        )
    rank_load.wait()
    for group in range(1, local_bits + 1):
        for copy in weight_loads(group):
            copy.start()
    for part in range(1, GROUP):
        load(part).start()
    for node in range(nodes):
        own_rank[node] = jnp.full(own_rank.shape[1:], ranks[0, node], jnp.int32)

    row = lax.broadcasted_iota(jnp.int32, (rank_rows, width), 0)

    def masked(values, rank_tile):
        return jnp.where(row < rank_tile[0:1, :], values, 0.0)

    def state(bank, chunk, node):
        return acc.at[chunk * nodes + node] if bank == 0 else tmp.at[chunk % GROUP, node]

    def stack(bank, pair, node, parts):
        halves = [split(state(bank, pair * GROUP + part, node)[...]) for part in parts]
        return tuple(jnp.concatenate(half, axis=1) for half in zip(*halves))

    def wide(weights, both):
        value = jnp.dot(weights, both, preferred_element_type=jnp.float32)
        return value[:, :width] + value[:, width:]

    def times(weights, stacked):
        if stacked[0].shape[1] == width:
            return wide(weights, jnp.concatenate(stacked, axis=1))
        return product(weights, stacked)

    def columns(values, at):
        return values[:, at * width : (at + 1) * width]

    def lower(level):
        return [node for node in range(nodes) if (node >> level) % 2 == 0]

    every = [(level, lower(level)) for level in range(local_bits)]
    early = every[:-1] + [(local_bits - 1, [0])]
    late = [(local_bits - 1, lower(local_bits - 1)[1:])]

    def local(pair, parts, stages):
        for level, chosen in stages:
            for node in chosen:
                other = node + (1 << level)
                mine, theirs = stack(level % 2, pair, node, parts), stack(level % 2, pair, other, parts)
                for to, at, source in ((node, mine, theirs), (other, theirs, mine)):
                    value = times(self_w[level, to], at)
                    value += times(cross_w[level, node + other - to], source)
                    for index, part in enumerate(parts):
                        state((level + 1) % 2, pair * GROUP + part, to)[...] = masked(
                            columns(value, index), own_rank[to]
                        )

    def first(step, parts):
        pair, node = step // nodes, step % nodes
        stacked = stack(local_bits % 2, pair, node, parts)
        value = times(cross_w[local_bits, node], stacked)
        for index, part in enumerate(parts):
            send[0, (pair * GROUP + part) * nodes + node] = columns(value, index)
            hop_copy(0, (pair * GROUP + part) * nodes + node).start()
        value = times(self_w[local_bits, node], stacked)
        for index, part in enumerate(parts):
            acc[(pair * GROUP + part) * nodes + node] = columns(value, index)

    def combine(hop, item, lead):
        level = local_bits + hop

        if level < len(bands):

            @pl.when(lead)
            def _():
                for copy in weight_loads(level):
                    copy.wait()

        hop_copy(hop - 1, item).wait_recv()
        node = item % nodes
        high, low = split(masked(acc[item] + recv[hop - 1, item], own_rank[node]))
        return node, level, jnp.concatenate([high, low], axis=1)

    def lanes(values, half):
        return values[:, half * (width // 2) : (half + 1) * (width // 2)]

    def fold(values):
        return jnp.concatenate([values[: rank_rows // 2], values[rank_rows // 2 :]], axis=1)

    def unfold(tile):
        return jnp.concatenate([lanes(tile, 0), lanes(tile, 1)], axis=0)

    def half_wide(weights, both, rank_tile):
        value = wide_dot(weights, both)
        value = lanes(value, 0) + lanes(value, 1)
        return jnp.where(row[:, : width // 2] < rank_tile[0:1, : width // 2], value, 0.0)

    def wide_dot(weights, both):
        return jnp.dot(weights, both, preferred_element_type=jnp.float32)

    def tail_last():
        item, node, level = items - 1, nodes - 1, levels - 1
        slots_in = [((pieces - 1) * (cols - 1) + step) * nodes + node for step in range(cols - 1)]
        for half in range(2):
            half_copy(0, half).wait_recv()
            value = lanes(acc[item], half) + unfold(tail_recv[0, half])
            value = jnp.where(row[:, : width // 2] < own_rank[node][0:1, : width // 2], value, 0.0)
            both = jnp.concatenate(split(value), axis=1)
            total = half_wide(cross_w[level, node], both, other_rank[node])
            for slot in slots_in:
                if half == 0:
                    col_copy(slot).wait_recv()
                total += lanes(col_recv[slot, 1], half)
            tail_send[1, half] = fold(total)
            half_copy(1, half).start()
            total = half_wide(self_w[level, node], both, own_rank[node])
            for slot in slots_in:
                total += lanes(col_recv[slot, 0], half)
            tail_keep[half] = total

    def tail_finish():
        values = []
        for half in range(2):
            half_copy(1, half).wait_recv()
            values.append(tail_keep[half] + unfold(tail_recv[1, half]))
        out[nodes - 1, :, pl.ds((pieces - 1) * width, width)] = jnp.concatenate(values, axis=1)

    def middle(hop, item, lead):
        node, level, parts = combine(hop, item, lead)
        value = wide(cross_w[level, node], parts)

        @pl.when((item < items - 1) | (hop < hops - 2))
        def _():
            send[hop, item] = value
            hop_copy(hop, item).start()

        if hop == hops - 2:

            @pl.when(item == items - 1)
            def _():
                for half in range(2):
                    tail_send[0, half] = fold(lanes(value, half))
                    half_copy(0, half).start()

        acc[item] = wide(self_w[level, node], parts)

    def last(item, lead):
        node, level, parts = combine(hops - 1, item, lead)

        @pl.when(lead)
        def _():
            rank_copy.wait()

        sent = masked(wide(cross_w[level, node], parts), other_rank[node])
        chunk = item // nodes
        piece = chunk // cols

        @pl.when(chunk % cols < cols - 1)
        def _():
            slot = (piece * (cols - 1) + chunk % cols) * nodes + node
            col_send[slot, 1] = sent
            col_send[slot, 0] = masked(wide(self_w[level, node], parts), own_rank[node])
            col_copy(slot).start()

        @pl.when(chunk % cols == cols - 1)
        def _():
            place = piece * nodes + node
            first_slot = piece * (cols - 1) * nodes + node
            total = sent
            for step in range(cols - 1):
                col_copy(first_slot + step * nodes).wait_recv()
                total += col_recv[first_slot + step * nodes, 1]
            end_send[place] = total
            end_copy(place).start()
            total = masked(wide(self_w[level, node], parts), own_rank[node])
            for step in range(cols - 1):
                total += col_recv[first_slot + step * nodes, 0]
            acc[item] = total

    def finish(item):
        node = item % nodes
        piece = item // (nodes * cols)
        place = piece * nodes + node
        end_copy(place).wait_recv()
        start = pl.multiple_of(piece * width, width)
        out[node, :, pl.ds(start, width)] = acc[item] + end_recv[place]

    steps = items // GROUP
    slots = GROUP * (steps + GROUP - 1)

    def lag(hop):
        return LAGS[0] + (min(hop, hops - 2) - 1) * LAGS[1] + sum(LAGS[2 : 4 + hop - hops])

    def place_of(slot):
        part = slot % GROUP
        step = slot // GROUP - part
        item = (step // nodes * GROUP + part) * nodes + step % nodes
        return (slot >= 0) & (step >= 0) & (step < steps), item

    load(0).wait()
    for level, chosen in early:
        for copy in weight_loads(level):
            copy.wait()
        local(0, (0,), [(level, chosen)])
    for group in range(local_bits + 1, len(bands)):
        for copy in weight_loads(group):
            copy.start()
    for copy in weight_loads(local_bits):
        copy.wait()
    pl.semaphore_wait(barrier, hops + cols - 1)
    rank_copy.start()
    first(0, (0,))
    for chunk in range(GROUP, chunks):
        load(chunk).start()
    local(0, (0,), late)
    def tick(time, _):
        step = time // GROUP

        @pl.when((time % GROUP == 0) & (step > 0) & (step < steps) & (step % nodes == 0))
        def _():
            @pl.when(step == nodes)
            def _():
                rest = pl.ds(GROUP * nodes, (chunks - GROUP) * nodes)
                pltpu.make_async_copy(acc.at[rest], acc.at[rest], load_sem.at[GROUP]).wait()

            local(step // nodes, tuple(range(GROUP)), every)

        @pl.when((time % GROUP == 0) & (step > 0) & (step < steps))
        def _():
            first(step, tuple(range(GROUP)))

        for hop in range(1, hops):
            slot = time - lag(hop)
            held, item = place_of(slot)

            if hop == hops - 1:

                @pl.when(held & (item < items - 1))
                def _():
                    last(item, slot == 0)

                @pl.when(held & (item == items - 1))
                def _():
                    tail_last()

            else:

                @pl.when(held)
                def _():
                    middle(hop, item, slot == 0)

        @pl.when(time == LAGS[0])
        def _():
            for part in range(1, GROUP):
                load(part).wait()
                local(0, (part,), every)
                first(0, (part,))

        slot = time - lag(hops)
        held, item = place_of(slot)

        @pl.when(held & ((item // nodes) % cols == cols - 1) & (item < items - 1))
        def _():
            finish(item)

        @pl.when(held & (item == items - 1))
        def _():
            tail_finish()

        return 0

    lax.fori_loop(0, slots + lag(hops), tick, 0)

    for hop in range(hops - 1):
        sent = pl.ds(0, items - hop // (hops - 2))
        whole_copy(send.at[hop, sent], recv.at[hop, sent], send_sem.at[hop], recv_sem.at[hop, 0]).wait_send()
    whole_copy(col_send, col_recv, col_send_sem, col_recv_sem.at[0, 0]).wait_send()
    sent = pl.ds(0, items - theirs - 1)
    whole_copy(end_send.at[sent], end_recv.at[sent], end_send_sem, end_recv_sem.at[0]).wait_send()
    for stage in range(2):
        for half in range(2):
            half_copy(stage, half).wait_send()


def shards(cols, coefficients, self_weights, cross_weights, true_ranks):
    nodes, rank, illum = coefficients.shape[1:]
    levels = self_weights.shape[1]
    shard = illum // cols
    width = min(WIDTH, shard)
    items = illum // width * nodes
    mine = shard // width * nodes
    theirs = items - mine
    hops = levels - (nodes.bit_length() - 1)
    tile = (rank, width)
    dma = pltpu.SemaphoreType.DMA
    return pl.pallas_call(
        functools.partial(kernel, cols, nodes, levels, width, shard),
        out_shape=jax.ShapeDtypeStruct((nodes, rank, shard), jnp.float32),
        in_specs=[pl.BlockSpec(memory_space=pl.ANY)] * 3 + [pl.BlockSpec(memory_space=pltpu.HBM)],
        out_specs=pl.BlockSpec(memory_space=pltpu.VMEM),
        scratch_shapes=[
            pltpu.VMEM((items, *tile), jnp.float32),
            pltpu.VMEM((GROUP, nodes, *tile), jnp.float32),
            pltpu.VMEM((levels, nodes, rank, rank), jnp.bfloat16),
            pltpu.VMEM((levels, nodes, rank, rank), jnp.bfloat16),
            pltpu.VMEM((hops - 1, items, *tile), jnp.float32),
            pltpu.VMEM((hops - 1, items, *tile), jnp.float32),
            pltpu.VMEM((theirs, 2, *tile), jnp.float32),
            pltpu.VMEM((theirs, 2, *tile), jnp.float32),
            pltpu.VMEM((mine, *tile), jnp.float32),
            pltpu.VMEM((mine, *tile), jnp.float32),
            pltpu.VMEM((2, 2, rank // 2, width), jnp.float32),
            pltpu.VMEM((2, 2, rank // 2, width), jnp.float32),
            pltpu.VMEM((2, rank, width // 2), jnp.float32),
            pltpu.SMEM(true_ranks.shape, jnp.int32),
            pltpu.VMEM((nodes, 8, width), jnp.int32),
            pltpu.VMEM((nodes, 8, width), jnp.int32),
            dma((GROUP + 1,)),
            dma((2, nodes.bit_length() + 2)),
            dma((hops - 1,)),
            dma((hops - 1, RING)),
            dma,
            dma((cols - 1, min(COL_RING, mine))),
            dma,
            dma((mine,)),
            dma((2,)),
            dma,
            dma((2, 2, 2)),
        ],
        compiler_params=pltpu.CompilerParams(
            collective_id=0, has_side_effects=True, vmem_limit_bytes=53 * 1024 * 1024
        ),
    )(coefficients, self_weights, cross_weights, pltpu.with_memory_space_constraint(true_ranks, pltpu.HBM))


def solution(mesh):
    placed = (
        P("col", "node", None, None),
        P("col", None, "node", None, None),
        P("col", None, "node", None, None),
        P("col", "node"),
    )
    return jax.shard_map(
        functools.partial(shards, mesh.shape["col"]),
        mesh=mesh, in_specs=placed, out_specs=P("node", None, "col"), check_vma=False,
    )
```

```python
import functools

import jax
import jax.numpy as jnp
from jax import lax
from jax.experimental import pallas as pl
from jax.experimental.pallas import tpu as pltpu
from jax.sharding import PartitionSpec as P

WIDTH = 128
GROUP = 2
RING = 12
COL_RING = 8
LAGS = (1, 3, 4, 16)


def flip(index, mask):
    return index + mask * (1 - 2 * ((index // mask) % 2))


def split(state):
    high = state.astype(jnp.bfloat16)
    low = (state - high.astype(jnp.float32)).astype(jnp.bfloat16)
    return high, low


def product(weights, parts):
    high, low = parts
    return jnp.dot(weights, high, preferred_element_type=jnp.float32) + jnp.dot(
        weights, low, preferred_element_type=jnp.float32
    )


def kernel(
    cols, nodes, levels, width, shard,
    coeff, self_hbm, cross_hbm, ranks_hbm, out,
    acc, tmp, self_w, cross_w, send, recv, col_send, col_recv, end_send, end_recv,
    tail_send, tail_recv,
    ranks, own_rank, other_rank,
    load_sem, weight_sem, send_sem, recv_sem, col_send_sem, col_recv_sem,
    end_send_sem, end_recv_sem, rank_sem, rank_load_sem, tail_sem,
):
    rank_rows = acc.shape[1]
    local_bits = nodes.bit_length() - 1
    hops = levels - local_bits
    pieces = shard // width
    chunks = cols * pieces
    items = chunks * nodes
    theirs = (cols - 1) * pieces * nodes
    me = lax.axis_index("node")
    my_col = lax.axis_index("col")
    peers = [flip(me, 1 << hop) for hop in range(hops)]

    def load(chunk):
        column = (my_col + 1 + chunk % cols) % cols
        start = pl.multiple_of(column * shard + (chunk // cols) * width, width)
        return pltpu.make_async_copy(
            coeff.at[0, :, :, pl.ds(start, width)],
            acc.at[pl.ds(chunk * nodes, nodes)],
            load_sem.at[min(chunk, GROUP)],
        )

    bands = [(level, level + 1) for level in range(local_bits + 2)] + [(local_bits + 2, levels)]

    def weight_loads(group):
        band = pl.ds(bands[group][0], bands[group][1] - bands[group][0])
        return (
            pltpu.make_async_copy(self_hbm.at[0, band], self_w.at[band], weight_sem.at[0, group]),
            pltpu.make_async_copy(cross_hbm.at[0, band], cross_w.at[band], weight_sem.at[1, group]),
        )

    def ring(item):
        chunk = item // nodes
        part = chunk % GROUP
        return (GROUP * (chunk // GROUP * nodes + item % nodes + part) + part) % RING

    def hop_copy(hop, item):
        return pltpu.make_async_remote_copy(
            src_ref=send.at[hop, item],
            dst_ref=recv.at[hop, item],
            send_sem=send_sem.at[hop],
            recv_sem=recv_sem.at[hop, ring(item)],
            device_id={"node": peers[hop]},
            device_id_type=pl.DeviceIdType.MESH,
        )

    def whole_copy(source, target, source_sem, target_sem):
        return pltpu.make_async_remote_copy(
            src_ref=source,
            dst_ref=target,
            send_sem=source_sem,
            recv_sem=target_sem,
            device_id={"node": peers[0]},
            device_id_type=pl.DeviceIdType.MESH,
        )

    def half_copy(stage, half):
        return pltpu.make_async_remote_copy(
            src_ref=tail_send.at[stage, half],
            dst_ref=tail_recv.at[stage, half],
            send_sem=tail_sem.at[0, stage, half],
            recv_sem=tail_sem.at[1, stage, half],
            device_id={"node": peers[hops - 2 + stage]},
            device_id_type=pl.DeviceIdType.MESH,
        )

    def col_copy(item):
        column = (my_col + 1 + (item // nodes) % (cols - 1)) % cols
        return pltpu.make_async_remote_copy(
            src_ref=col_send.at[item],
            dst_ref=col_recv.at[item],
            send_sem=col_send_sem,
            recv_sem=col_recv_sem.at[item // nodes % (cols - 1), (item // nodes // (cols - 1) * nodes + item % nodes) % col_recv_sem.shape[1]],
            device_id={"col": column},
            device_id_type=pl.DeviceIdType.MESH,
        )

    def end_copy(place):
        return pltpu.make_async_remote_copy(
            src_ref=end_send.at[place],
            dst_ref=end_recv.at[place],
            send_sem=end_send_sem,
            recv_sem=end_recv_sem.at[place],
            device_id={"node": peers[hops - 1]},
            device_id_type=pl.DeviceIdType.MESH,
        )

    rank_copy = pltpu.make_async_remote_copy(
        src_ref=own_rank,
        dst_ref=other_rank,
        send_sem=rank_sem.at[0],
        recv_sem=rank_sem.at[1],
        device_id={"node": peers[hops - 1]},
        device_id_type=pl.DeviceIdType.MESH,
    )

    rank_load = pltpu.make_async_copy(ranks_hbm, ranks, rank_load_sem)
    rank_load.start()
    load(0).start()
    for copy in weight_loads(0):
        copy.start()

    barrier = pltpu.get_barrier_semaphore()
    for peer in peers:
        pl.semaphore_signal(barrier, inc=1, device_id={"node": peer}, device_id_type=pl.DeviceIdType.MESH)
    for step in range(1, cols):
        pl.semaphore_signal(
            barrier, inc=1, device_id={"col": (my_col + step) % cols}, device_id_type=pl.DeviceIdType.MESH
        )
    rank_load.wait()
    for group in range(1, local_bits + 1):
        for copy in weight_loads(group):
            copy.start()
    for part in range(1, GROUP):
        load(part).start()
    for node in range(nodes):
        own_rank[node] = jnp.full(own_rank.shape[1:], ranks[0, node], jnp.int32)

    row = lax.broadcasted_iota(jnp.int32, (rank_rows, width), 0)

    def masked(values, rank_tile):
        return jnp.where(row < rank_tile[0:1, :], values, 0.0)

    def state(bank, chunk, node):
        return acc.at[chunk * nodes + node] if bank == 0 else tmp.at[chunk % GROUP, node]

    def stack(bank, pair, node, parts):
        halves = [split(state(bank, pair * GROUP + part, node)[...]) for part in parts]
        return tuple(jnp.concatenate(half, axis=1) for half in zip(*halves))

    def wide(weights, both):
        value = jnp.dot(weights, both, preferred_element_type=jnp.float32)
        return value[:, :width] + value[:, width:]

    def times(weights, stacked):
        if stacked[0].shape[1] == width:
            return wide(weights, jnp.concatenate(stacked, axis=1))
        return product(weights, stacked)

    def columns(values, at):
        return values[:, at * width : (at + 1) * width]

    def lower(level):
        return [node for node in range(nodes) if (node >> level) % 2 == 0]

    every = [(level, lower(level)) for level in range(local_bits)]
    early = every[:-1] + [(local_bits - 1, [0])]
    late = [(local_bits - 1, lower(local_bits - 1)[1:])]

    def local(pair, parts, stages):
        for level, chosen in stages:
            for node in chosen:
                other = node + (1 << level)
                mine, theirs = stack(level % 2, pair, node, parts), stack(level % 2, pair, other, parts)
                for to, at, source in ((node, mine, theirs), (other, theirs, mine)):
                    value = times(self_w[level, to], at)
                    value += times(cross_w[level, node + other - to], source)
                    for index, part in enumerate(parts):
                        state((level + 1) % 2, pair * GROUP + part, to)[...] = masked(
                            columns(value, index), own_rank[to]
                        )

    def first(step, parts):
        pair, node = step // nodes, step % nodes
        stacked = stack(local_bits % 2, pair, node, parts)
        value = times(cross_w[local_bits, node], stacked)
        for index, part in enumerate(parts):
            send[0, (pair * GROUP + part) * nodes + node] = columns(value, index)
            hop_copy(0, (pair * GROUP + part) * nodes + node).start()
        value = times(self_w[local_bits, node], stacked)
        for index, part in enumerate(parts):
            acc[(pair * GROUP + part) * nodes + node] = columns(value, index)

    def combine(hop, item, lead):
        level = local_bits + hop

        if level < len(bands):

            @pl.when(lead)
            def _():
                for copy in weight_loads(level):
                    copy.wait()

        hop_copy(hop - 1, item).wait_recv()
        node = item % nodes
        high, low = split(masked(acc[item] + recv[hop - 1, item], own_rank[node]))
        return node, level, jnp.concatenate([high, low], axis=1)

    def lanes(values, half):
        return values[:, half * (width // 2) : (half + 1) * (width // 2)]

    def fold(values):
        return jnp.concatenate([values[: rank_rows // 2], values[rank_rows // 2 :]], axis=1)

    def unfold(tile):
        return jnp.concatenate([lanes(tile, 0), lanes(tile, 1)], axis=0)

    def half_wide(weights, both, rank_tile):
        value = wide_dot(weights, both)
        value = lanes(value, 0) + lanes(value, 1)
        return jnp.where(row[:, : width // 2] < rank_tile[0:1, : width // 2], value, 0.0)

    def wide_dot(weights, both):
        return jnp.dot(weights, both, preferred_element_type=jnp.float32)

    def tail_last():
        item, node, level = items - 1, nodes - 1, levels - 1
        slots_in = [((pieces - 1) * (cols - 1) + step) * nodes + node for step in range(cols - 1)]
        for half in range(2):
            half_copy(0, half).wait_recv()
            value = lanes(acc[item], half) + unfold(tail_recv[0, half])
            value = jnp.where(row[:, : width // 2] < own_rank[node][0:1, : width // 2], value, 0.0)
            both = jnp.concatenate(split(value), axis=1)
            total = half_wide(cross_w[level, node], both, other_rank[node])
            for slot in slots_in:
                if half == 0:
                    col_copy(slot).wait_recv()
                total += lanes(col_recv[slot, 1], half)
            tail_send[1, half] = fold(total)
            half_copy(1, half).start()
            total = half_wide(self_w[level, node], both, own_rank[node])
            for slot in slots_in:
                total += lanes(col_recv[slot, 0], half)
            tmp[half, 0, pl.ds(0, rank_rows // 2)] = fold(total)

    def tail_finish():
        values = []
        for half in range(2):
            half_copy(1, half).wait_recv()
            values.append(unfold(tmp[half, 0, pl.ds(0, rank_rows // 2)] + tail_recv[1, half]))
        out[nodes - 1, :, pl.ds((pieces - 1) * width, width)] = jnp.concatenate(values, axis=1)

    def middle(hop, item, lead):
        node, level, parts = combine(hop, item, lead)
        value = wide(cross_w[level, node], parts)

        @pl.when((item < items - 1) | (hop < hops - 2))
        def _():
            send[hop, item] = value
            hop_copy(hop, item).start()

        if hop == hops - 2:

            @pl.when(item == items - 1)
            def _():
                for half in range(2):
                    tail_send[0, half] = fold(lanes(value, half))
                    half_copy(0, half).start()

        acc[item] = wide(self_w[level, node], parts)

    def last(item, lead):
        node, level, parts = combine(hops - 1, item, lead)

        @pl.when(lead)
        def _():
            rank_copy.wait()

        sent = masked(wide(cross_w[level, node], parts), other_rank[node])
        chunk = item // nodes
        piece = chunk // cols

        @pl.when(chunk % cols < cols - 1)
        def _():
            slot = (piece * (cols - 1) + chunk % cols) * nodes + node
            col_send[slot, 1] = sent
            col_send[slot, 0] = masked(wide(self_w[level, node], parts), own_rank[node])
            col_copy(slot).start()

        @pl.when(chunk % cols == cols - 1)
        def _():
            place = piece * nodes + node
            first_slot = piece * (cols - 1) * nodes + node
            total = sent
            for step in range(cols - 1):
                col_copy(first_slot + step * nodes).wait_recv()
                total += col_recv[first_slot + step * nodes, 1]
            end_send[place] = total
            end_copy(place).start()
            total = masked(wide(self_w[level, node], parts), own_rank[node])
            for step in range(cols - 1):
                total += col_recv[first_slot + step * nodes, 0]
            acc[item] = total

    def finish(item):
        node = item % nodes
        piece = item // (nodes * cols)
        place = piece * nodes + node
        end_copy(place).wait_recv()
        start = pl.multiple_of(piece * width, width)
        out[node, :, pl.ds(start, width)] = acc[item] + end_recv[place]

    steps = items // GROUP
    slots = GROUP * (steps + GROUP - 1)

    def lag(hop):
        return LAGS[0] + (min(hop, hops - 2) - 1) * LAGS[1] + sum(LAGS[2 : 4 + hop - hops])

    def place_of(slot):
        part = slot % GROUP
        step = slot // GROUP - part
        item = (step // nodes * GROUP + part) * nodes + step % nodes
        return (slot >= 0) & (step >= 0) & (step < steps), item

    load(0).wait()
    for level, chosen in early:
        for copy in weight_loads(level):
            copy.wait()
        local(0, (0,), [(level, chosen)])
    for group in range(local_bits + 1, len(bands)):
        for copy in weight_loads(group):
            copy.start()
    for copy in weight_loads(local_bits):
        copy.wait()
    pl.semaphore_wait(barrier, hops + cols - 1)
    rank_copy.start()
    first(0, (0,))
    for chunk in range(GROUP, chunks):
        load(chunk).start()
    local(0, (0,), late)
    def tick(time, _):
        step = time // GROUP

        @pl.when((time % GROUP == 0) & (step > 0) & (step < steps) & (step % nodes == 0))
        def _():
            @pl.when(step == nodes)
            def _():
                rest = pl.ds(GROUP * nodes, (chunks - GROUP) * nodes)
                pltpu.make_async_copy(acc.at[rest], acc.at[rest], load_sem.at[GROUP]).wait()

            local(step // nodes, tuple(range(GROUP)), every)

        @pl.when((time % GROUP == 0) & (step > 0) & (step < steps))
        def _():
            first(step, tuple(range(GROUP)))

        for hop in range(1, hops):
            slot = time - lag(hop)
            held, item = place_of(slot)

            if hop == hops - 1:

                @pl.when(held & (item < items - 1))
                def _():
                    last(item, slot == 0)

                @pl.when(held & (item == items - 1))
                def _():
                    tail_last()

            else:

                @pl.when(held)
                def _():
                    middle(hop, item, slot == 0)

        @pl.when(time == LAGS[0])
        def _():
            for part in range(1, GROUP):
                load(part).wait()
                local(0, (part,), every)
                first(0, (part,))

        slot = time - lag(hops)
        held, item = place_of(slot)

        @pl.when(held & ((item // nodes) % cols == cols - 1) & (item < items - 1))
        def _():
            finish(item)

        @pl.when(held & (item == items - 1))
        def _():
            tail_finish()

        return 0

    lax.fori_loop(0, slots + lag(hops), tick, 0)

    for hop in range(hops - 1):
        sent = pl.ds(0, items - hop // (hops - 2))
        whole_copy(send.at[hop, sent], recv.at[hop, sent], send_sem.at[hop], recv_sem.at[hop, 0]).wait_send()
    whole_copy(col_send, col_recv, col_send_sem, col_recv_sem.at[0, 0]).wait_send()
    sent = pl.ds(0, items - theirs - 1)
    whole_copy(end_send.at[sent], end_recv.at[sent], end_send_sem, end_recv_sem.at[0]).wait_send()
    for stage in range(2):
        for half in range(2):
            half_copy(stage, half).wait_send()


def shards(cols, coefficients, self_weights, cross_weights, true_ranks):
    nodes, rank, illum = coefficients.shape[1:]
    levels = self_weights.shape[1]
    shard = illum // cols
    width = min(WIDTH, shard)
    items = illum // width * nodes
    mine = shard // width * nodes
    theirs = items - mine
    hops = levels - (nodes.bit_length() - 1)
    tile = (rank, width)
    dma = pltpu.SemaphoreType.DMA
    return pl.pallas_call(
        functools.partial(kernel, cols, nodes, levels, width, shard),
        out_shape=jax.ShapeDtypeStruct((nodes, rank, shard), jnp.float32),
        in_specs=[pl.BlockSpec(memory_space=pl.ANY)] * 3 + [pl.BlockSpec(memory_space=pltpu.HBM)],
        out_specs=pl.BlockSpec(memory_space=pltpu.VMEM),
        scratch_shapes=[
            pltpu.VMEM((items, *tile), jnp.float32),
            pltpu.VMEM((GROUP, nodes, *tile), jnp.float32),
            pltpu.VMEM((levels, nodes, rank, rank), jnp.bfloat16),
            pltpu.VMEM((levels, nodes, rank, rank), jnp.bfloat16),
            pltpu.VMEM((hops - 1, items, *tile), jnp.float32),
            pltpu.VMEM((hops - 1, items, *tile), jnp.float32),
            pltpu.VMEM((theirs, 2, *tile), jnp.float32),
            pltpu.VMEM((theirs, 2, *tile), jnp.float32),
            pltpu.VMEM((mine, *tile), jnp.float32),
            pltpu.VMEM((mine, *tile), jnp.float32),
            pltpu.VMEM((2, 2, rank // 2, width), jnp.float32),
            pltpu.VMEM((2, 2, rank // 2, width), jnp.float32),
            pltpu.SMEM(true_ranks.shape, jnp.int32),
            pltpu.VMEM((nodes, 8, width), jnp.int32),
            pltpu.VMEM((nodes, 8, width), jnp.int32),
            dma((GROUP + 1,)),
            dma((2, nodes.bit_length() + 2)),
            dma((hops - 1,)),
            dma((hops - 1, RING)),
            dma,
            dma((cols - 1, min(COL_RING, mine))),
            dma,
            dma((mine,)),
            dma((2,)),
            dma,
            dma((2, 2, 2)),
        ],
        compiler_params=pltpu.CompilerParams(
            collective_id=0, has_side_effects=True, vmem_limit_bytes=53 * 1024 * 1024 - nodes * rank * shard * 4
        ),
    )(coefficients, self_weights, cross_weights, pltpu.with_memory_space_constraint(true_ranks, pltpu.HBM))


def solution(mesh):
    placed = (
        P("col", "node", None, None),
        P("col", None, "node", None, None),
        P("col", None, "node", None, None),
        P("col", "node"),
    )
    return jax.shard_map(
        functools.partial(shards, mesh.shape["col"]),
        mesh=mesh, in_specs=placed, out_specs=P("node", None, "col"), check_vma=False,
    )
```

```python
import functools

import jax
import jax.numpy as jnp
from jax import lax
from jax.experimental import pallas as pl
from jax.experimental.pallas import tpu as pltpu
from jax.sharding import PartitionSpec as P

WIDTH = 128
GROUP = 2
RING = 14
COL_RING = 8
LAGS = (1, 3, 5, 14)


def flip(index, mask):
    return index + mask * (1 - 2 * ((index // mask) % 2))


def split(state):
    high = state.astype(jnp.bfloat16)
    low = (state - high.astype(jnp.float32)).astype(jnp.bfloat16)
    return high, low


def product(weights, parts):
    high, low = parts
    return jnp.dot(weights, high, preferred_element_type=jnp.float32) + jnp.dot(
        weights, low, preferred_element_type=jnp.float32
    )


def kernel(
    cols, nodes, levels, width, shard,
    coeff, self_hbm, cross_hbm, ranks_hbm, out,
    acc, tmp, self_w, cross_w, send, recv, col_send, col_recv, end_send, end_recv,
    tail_send, tail_recv,
    ranks, own_rank, other_rank,
    load_sem, weight_sem, send_sem, recv_sem, col_send_sem, col_recv_sem,
    end_send_sem, end_recv_sem, rank_sem, rank_load_sem, tail_sem,
):
    rank_rows = acc.shape[1]
    local_bits = nodes.bit_length() - 1
    hops = levels - local_bits
    pieces = shard // width
    chunks = cols * pieces
    items = chunks * nodes
    theirs = (cols - 1) * pieces * nodes
    me = lax.axis_index("node")
    my_col = lax.axis_index("col")
    peers = [flip(me, 1 << hop) for hop in range(hops)]

    def load(chunk):
        column = (my_col + 1 + chunk % cols) % cols
        start = pl.multiple_of(column * shard + (chunk // cols) * width, width)
        return pltpu.make_async_copy(
            coeff.at[0, :, :, pl.ds(start, width)],
            acc.at[pl.ds(chunk * nodes, nodes)],
            load_sem.at[min(chunk, GROUP)],
        )

    bands = [(level, level + 1) for level in range(local_bits + 2)] + [(local_bits + 2, levels)]

    def weight_loads(group):
        band = pl.ds(bands[group][0], bands[group][1] - bands[group][0])
        return (
            pltpu.make_async_copy(self_hbm.at[0, band], self_w.at[band], weight_sem.at[0, group]),
            pltpu.make_async_copy(cross_hbm.at[0, band], cross_w.at[band], weight_sem.at[1, group]),
        )

    def ring(item):
        chunk = item // nodes
        part = chunk % GROUP
        return (GROUP * (chunk // GROUP * nodes + item % nodes + part) + part) % RING

    def hop_copy(hop, item):
        return pltpu.make_async_remote_copy(
            src_ref=send.at[hop, item],
            dst_ref=recv.at[hop, item],
            send_sem=send_sem.at[hop],
            recv_sem=recv_sem.at[hop, ring(item)],
            device_id={"node": peers[hop]},
            device_id_type=pl.DeviceIdType.MESH,
        )

    def whole_copy(source, target, source_sem, target_sem):
        return pltpu.make_async_remote_copy(
            src_ref=source,
            dst_ref=target,
            send_sem=source_sem,
            recv_sem=target_sem,
            device_id={"node": peers[0]},
            device_id_type=pl.DeviceIdType.MESH,
        )

    def half_copy(stage, half):
        return pltpu.make_async_remote_copy(
            src_ref=tail_send.at[stage, half],
            dst_ref=tail_recv.at[stage, half],
            send_sem=tail_sem.at[0, stage, half],
            recv_sem=tail_sem.at[1, stage, half],
            device_id={"node": peers[hops - 2 + stage]},
            device_id_type=pl.DeviceIdType.MESH,
        )

    def col_copy(item):
        column = (my_col + 1 + (item // nodes) % (cols - 1)) % cols
        return pltpu.make_async_remote_copy(
            src_ref=col_send.at[item],
            dst_ref=col_recv.at[item],
            send_sem=col_send_sem,
            recv_sem=col_recv_sem.at[item // nodes % (cols - 1), (item // nodes // (cols - 1) * nodes + item % nodes) % col_recv_sem.shape[1]],
            device_id={"col": column},
            device_id_type=pl.DeviceIdType.MESH,
        )

    def end_copy(place):
        return pltpu.make_async_remote_copy(
            src_ref=end_send.at[place],
            dst_ref=end_recv.at[place],
            send_sem=end_send_sem,
            recv_sem=end_recv_sem.at[place],
            device_id={"node": peers[hops - 1]},
            device_id_type=pl.DeviceIdType.MESH,
        )

    rank_copy = pltpu.make_async_remote_copy(
        src_ref=own_rank,
        dst_ref=other_rank,
        send_sem=rank_sem.at[0],
        recv_sem=rank_sem.at[1],
        device_id={"node": peers[hops - 1]},
        device_id_type=pl.DeviceIdType.MESH,
    )

    rank_load = pltpu.make_async_copy(ranks_hbm, ranks, rank_load_sem)
    rank_load.start()
    load(0).start()
    for copy in weight_loads(0):
        copy.start()

    barrier = pltpu.get_barrier_semaphore()
    for peer in peers:
        pl.semaphore_signal(barrier, inc=1, device_id={"node": peer}, device_id_type=pl.DeviceIdType.MESH)
    for step in range(1, cols):
        pl.semaphore_signal(
            barrier, inc=1, device_id={"col": (my_col + step) % cols}, device_id_type=pl.DeviceIdType.MESH
        )
    rank_load.wait()
    for group in range(1, local_bits + 1):
        for copy in weight_loads(group):
            copy.start()
    for part in range(1, GROUP):
        load(part).start()
    for node in range(nodes):
        own_rank[node] = jnp.full(own_rank.shape[1:], ranks[0, node], jnp.int32)

    row = lax.broadcasted_iota(jnp.int32, (rank_rows, width), 0)

    def masked(values, rank_tile):
        return jnp.where(row < rank_tile[0:1, :], values, 0.0)

    def state(bank, chunk, node):
        return acc.at[chunk * nodes + node] if bank == 0 else tmp.at[chunk % GROUP, node]

    def stack(bank, pair, node, parts):
        halves = [split(state(bank, pair * GROUP + part, node)[...]) for part in parts]
        return tuple(jnp.concatenate(half, axis=1) for half in zip(*halves))

    def wide(weights, both):
        value = jnp.dot(weights, both, preferred_element_type=jnp.float32)
        return value[:, :width] + value[:, width:]

    def times(weights, stacked):
        if stacked[0].shape[1] == width:
            return wide(weights, jnp.concatenate(stacked, axis=1))
        return product(weights, stacked)

    def columns(values, at):
        return values[:, at * width : (at + 1) * width]

    def lower(level):
        return [node for node in range(nodes) if (node >> level) % 2 == 0]

    every = [(level, lower(level)) for level in range(local_bits)]
    early = every[:-1] + [(local_bits - 1, [0])]
    late = [(local_bits - 1, lower(local_bits - 1)[1:])]

    def local(pair, parts, stages):
        for level, chosen in stages:
            for node in chosen:
                other = node + (1 << level)
                mine, theirs = stack(level % 2, pair, node, parts), stack(level % 2, pair, other, parts)
                for to, at, source in ((node, mine, theirs), (other, theirs, mine)):
                    value = times(self_w[level, to], at)
                    value += times(cross_w[level, node + other - to], source)
                    for index, part in enumerate(parts):
                        state((level + 1) % 2, pair * GROUP + part, to)[...] = masked(
                            columns(value, index), own_rank[to]
                        )

    def first(step, parts):
        pair, node = step // nodes, step % nodes
        stacked = stack(local_bits % 2, pair, node, parts)
        value = times(cross_w[local_bits, node], stacked)
        for index, part in enumerate(parts):
            send[0, (pair * GROUP + part) * nodes + node] = columns(value, index)
            hop_copy(0, (pair * GROUP + part) * nodes + node).start()
        value = times(self_w[local_bits, node], stacked)
        for index, part in enumerate(parts):
            acc[(pair * GROUP + part) * nodes + node] = columns(value, index)

    def combine(hop, item, lead):
        level = local_bits + hop

        if level < len(bands):

            @pl.when(lead)
            def _():
                for copy in weight_loads(level):
                    copy.wait()

        hop_copy(hop - 1, item).wait_recv()
        node = item % nodes
        high, low = split(masked(acc[item] + recv[hop - 1, item], own_rank[node]))
        return node, level, jnp.concatenate([high, low], axis=1)

    def lanes(values, half):
        return values[:, half * (width // 2) : (half + 1) * (width // 2)]

    def fold(values):
        return jnp.concatenate([values[: rank_rows // 2], values[rank_rows // 2 :]], axis=1)

    def unfold(tile):
        return jnp.concatenate([lanes(tile, 0), lanes(tile, 1)], axis=0)

    def half_wide(weights, both, rank_tile):
        value = wide_dot(weights, both)
        value = lanes(value, 0) + lanes(value, 1)
        return jnp.where(row[:, : width // 2] < rank_tile[0:1, : width // 2], value, 0.0)

    def wide_dot(weights, both):
        return jnp.dot(weights, both, preferred_element_type=jnp.float32)

    def tail_last():
        item, node, level = items - 1, nodes - 1, levels - 1
        slots_in = [((pieces - 1) * (cols - 1) + step) * nodes + node for step in range(cols - 1)]
        for half in range(2):
            half_copy(0, half).wait_recv()
            value = lanes(acc[item], half) + unfold(tail_recv[0, half])
            value = jnp.where(row[:, : width // 2] < own_rank[node][0:1, : width // 2], value, 0.0)
            both = jnp.concatenate(split(value), axis=1)
            total = half_wide(cross_w[level, node], both, other_rank[node])
            for slot in slots_in:
                if half == 0:
                    col_copy(slot).wait_recv()
                total += lanes(col_recv[slot, 1], half)
            tail_send[1, half] = fold(total)
            half_copy(1, half).start()
            total = half_wide(self_w[level, node], both, own_rank[node])
            for slot in slots_in:
                total += lanes(col_recv[slot, 0], half)
            tmp[half, 0, pl.ds(0, rank_rows // 2)] = fold(total)

    def tail_finish():
        values = []
        for half in range(2):
            half_copy(1, half).wait_recv()
            values.append(unfold(tmp[half, 0, pl.ds(0, rank_rows // 2)] + tail_recv[1, half]))
        out[nodes - 1, :, pl.ds((pieces - 1) * width, width)] = jnp.concatenate(values, axis=1)

    def middle(hop, item, lead):
        node, level, parts = combine(hop, item, lead)
        value = wide(cross_w[level, node], parts)

        @pl.when((item < items - 1) | (hop < hops - 2))
        def _():
            send[hop, item] = value
            hop_copy(hop, item).start()

        if hop == hops - 2:

            @pl.when(item == items - 1)
            def _():
                for half in range(2):
                    tail_send[0, half] = fold(lanes(value, half))
                    half_copy(0, half).start()

        acc[item] = wide(self_w[level, node], parts)

    def last(item, lead):
        node, level, parts = combine(hops - 1, item, lead)

        @pl.when(lead)
        def _():
            rank_copy.wait()

        sent = masked(wide(cross_w[level, node], parts), other_rank[node])
        chunk = item // nodes
        piece = chunk // cols

        @pl.when(chunk % cols < cols - 1)
        def _():
            slot = (piece * (cols - 1) + chunk % cols) * nodes + node
            col_send[slot, 1] = sent
            col_send[slot, 0] = masked(wide(self_w[level, node], parts), own_rank[node])
            col_copy(slot).start()

        @pl.when(chunk % cols == cols - 1)
        def _():
            place = piece * nodes + node
            first_slot = piece * (cols - 1) * nodes + node
            total = sent
            for step in range(cols - 1):
                col_copy(first_slot + step * nodes).wait_recv()
                total += col_recv[first_slot + step * nodes, 1]
            end_send[place] = total
            end_copy(place).start()
            total = masked(wide(self_w[level, node], parts), own_rank[node])
            for step in range(cols - 1):
                total += col_recv[first_slot + step * nodes, 0]
            acc[item] = total

    def finish(item):
        node = item % nodes
        piece = item // (nodes * cols)
        place = piece * nodes + node
        end_copy(place).wait_recv()
        start = pl.multiple_of(piece * width, width)
        out[node, :, pl.ds(start, width)] = acc[item] + end_recv[place]

    steps = items // GROUP
    slots = GROUP * (steps + GROUP - 1)

    def lag(hop):
        return LAGS[0] + (min(hop, hops - 2) - 1) * LAGS[1] + sum(LAGS[2 : 4 + hop - hops])

    def place_of(slot):
        part = slot % GROUP
        step = slot // GROUP - part
        item = (step // nodes * GROUP + part) * nodes + step % nodes
        return (slot >= 0) & (step >= 0) & (step < steps), item

    load(0).wait()
    for level, chosen in early:
        for copy in weight_loads(level):
            copy.wait()
        local(0, (0,), [(level, chosen)])
    for group in range(local_bits + 1, len(bands)):
        for copy in weight_loads(group):
            copy.start()
    for copy in weight_loads(local_bits):
        copy.wait()
    pl.semaphore_wait(barrier, hops + cols - 1)
    rank_copy.start()
    first(0, (0,))
    for chunk in range(GROUP, chunks):
        load(chunk).start()
    local(0, (0,), late)
    def tick(time, _):
        step = time // GROUP

        @pl.when((time % GROUP == 0) & (step > 0) & (step < steps) & (step % nodes == 0))
        def _():
            @pl.when(step == nodes)
            def _():
                rest = pl.ds(GROUP * nodes, (chunks - GROUP) * nodes)
                pltpu.make_async_copy(acc.at[rest], acc.at[rest], load_sem.at[GROUP]).wait()

            local(step // nodes, tuple(range(GROUP)), every)

        @pl.when((time % GROUP == 0) & (step > 0) & (step < steps))
        def _():
            first(step, tuple(range(GROUP)))

        for hop in range(1, hops):
            slot = time - lag(hop)
            held, item = place_of(slot)

            if hop == hops - 1:

                @pl.when(held & (item < items - 1))
                def _():
                    last(item, slot == 0)

                @pl.when(held & (item == items - 1))
                def _():
                    tail_last()

            else:

                @pl.when(held)
                def _():
                    middle(hop, item, slot == 0)

        @pl.when(time == LAGS[0])
        def _():
            for part in range(1, GROUP):
                load(part).wait()
                local(0, (part,), every)
                first(0, (part,))

        slot = time - lag(hops)
        held, item = place_of(slot)

        @pl.when(held & ((item // nodes) % cols == cols - 1) & (item < items - 1))
        def _():
            finish(item)

        @pl.when(held & (item == items - 1))
        def _():
            tail_finish()

        return 0

    lax.fori_loop(0, slots + lag(hops), tick, 0)

    for hop in range(hops - 1):
        sent = pl.ds(0, items - hop // (hops - 2))
        whole_copy(send.at[hop, sent], recv.at[hop, sent], send_sem.at[hop], recv_sem.at[hop, 0]).wait_send()
    whole_copy(col_send, col_recv, col_send_sem, col_recv_sem.at[0, 0]).wait_send()
    sent = pl.ds(0, items - theirs - 1)
    whole_copy(end_send.at[sent], end_recv.at[sent], end_send_sem, end_recv_sem.at[0]).wait_send()
    for stage in range(2):
        for half in range(2):
            half_copy(stage, half).wait_send()


def shards(cols, coefficients, self_weights, cross_weights, true_ranks):
    nodes, rank, illum = coefficients.shape[1:]
    levels = self_weights.shape[1]
    shard = illum // cols
    width = min(WIDTH, shard)
    items = illum // width * nodes
    mine = shard // width * nodes
    theirs = items - mine
    hops = levels - (nodes.bit_length() - 1)
    tile = (rank, width)
    dma = pltpu.SemaphoreType.DMA
    return pl.pallas_call(
        functools.partial(kernel, cols, nodes, levels, width, shard),
        out_shape=jax.ShapeDtypeStruct((nodes, rank, shard), jnp.float32),
        in_specs=[pl.BlockSpec(memory_space=pl.ANY)] * 3 + [pl.BlockSpec(memory_space=pltpu.HBM)],
        out_specs=pl.BlockSpec(memory_space=pltpu.VMEM),
        scratch_shapes=[
            pltpu.VMEM((items, *tile), jnp.float32),
            pltpu.VMEM((GROUP, nodes, *tile), jnp.float32),
            pltpu.VMEM((levels, nodes, rank, rank), jnp.bfloat16),
            pltpu.VMEM((levels, nodes, rank, rank), jnp.bfloat16),
            pltpu.VMEM((hops - 1, items, *tile), jnp.float32),
            pltpu.VMEM((hops - 1, items, *tile), jnp.float32),
            pltpu.VMEM((theirs, 2, *tile), jnp.float32),
            pltpu.VMEM((theirs, 2, *tile), jnp.float32),
            pltpu.VMEM((mine, *tile), jnp.float32),
            pltpu.VMEM((mine, *tile), jnp.float32),
            pltpu.VMEM((2, 2, rank // 2, width), jnp.float32),
            pltpu.VMEM((2, 2, rank // 2, width), jnp.float32),
            pltpu.SMEM(true_ranks.shape, jnp.int32),
            pltpu.VMEM((nodes, 8, width), jnp.int32),
            pltpu.VMEM((nodes, 8, width), jnp.int32),
            dma((GROUP + 1,)),
            dma((2, nodes.bit_length() + 2)),
            dma((hops - 1,)),
            dma((hops - 1, RING)),
            dma,
            dma((cols - 1, min(COL_RING, mine))),
            dma,
            dma((mine,)),
            dma((2,)),
            dma,
            dma((2, 2, 2)),
        ],
        compiler_params=pltpu.CompilerParams(
            collective_id=0, has_side_effects=True, vmem_limit_bytes=53 * 1024 * 1024 - nodes * rank * shard * 4
        ),
    )(coefficients, self_weights, cross_weights, pltpu.with_memory_space_constraint(true_ranks, pltpu.HBM))


def solution(mesh):
    placed = (
        P("col", "node", None, None),
        P("col", None, "node", None, None),
        P("col", None, "node", None, None),
        P("col", "node"),
    )
    return jax.shard_map(
        functools.partial(shards, mesh.shape["col"]),
        mesh=mesh, in_specs=placed, out_specs=P("node", None, "col"), check_vma=False,
    )
```
